8 devices in a mesh: rep: 2 (over y, z), dp: 4 (over x, core).
Axes of the slice: x: 2, y: 2, z: 1, core: 2. Of those that a mesh axis runs over, the one named last changes fastest.
Arguments:
- x: bfloat16 [8, 2048, 1024], P(('rep', 'dp')), parts along dimension 0
- dy: bfloat16 [8, 2048, 1024], P(('rep', 'dp')), parts along dimension 0
- w_gate: bfloat16 [2, 1024, 2816], replicated
- w_up: bfloat16 [2, 1024, 2816], replicated
- w_down: bfloat16 [2, 2816, 1024], replicated
- m_w_gate: float32 [2, 1024, 2816], P(None, 'dp')
- m_w_up: float32 [2, 1024, 2816], P(None, 'dp')
- m_w_down: float32 [2, 2816, 1024], P(None, 'dp')
- v_w_gate: float32 [2, 1024, 2816], P(None, 'dp')
- v_w_up: float32 [2, 1024, 2816], P(None, 'dp')
- v_w_down: float32 [2, 2816, 1024], P(None, 'dp')
Outputs:
- output 1: bfloat16 [4, 1024, 2816], P('rep'), parts along dimension 0
- output 2: bfloat16 [4, 1024, 2816], P('rep'), parts along dimension 0
- output 3: bfloat16 [4, 2816, 1024], P('rep'), parts along dimension 0
- output 4: float32 [4, 1024, 2816], P('rep', 'dp'), parts along dimension 0
- output 5: float32 [4, 1024, 2816], P('rep', 'dp'), parts along dimension 0
- output 6: float32 [4, 2816, 1024], P('rep', 'dp'), parts along dimension 0
- output 7: float32 [4, 1024, 2816], P('rep', 'dp'), parts along dimension 0
- output 8: float32 [4, 1024, 2816], P('rep', 'dp'), parts along dimension 0
- output 9: float32 [4, 2816, 1024], P('rep', 'dp'), parts along dimension 0
There are 2 independent parts. The reference program is written for one: setup_inputs(seed, part) draws one part's arguments, and reference() takes and returns one part's arrays. A program takes and returns all parts, laid end to end along the dimension named above; an argument that names none is the same for every part.
All inputs are finite; a program needn't handle non-finite values.
Results may differ from the reference program's by a relative error of at most 0.022.
Values are sent between devices in bfloat16 or wider.
A program may use at most 2 GiB of HBM per device.

```python
import jax
import jax.numpy as jnp
from jax import lax

SEQUENCES = 4
TOKENS = 2048
D = 1024
FF = 2816
LAYERS = 2
NAMES = ("w_gate", "w_up", "w_down")
SHAPES = {"w_gate": (LAYERS, D, FF), "w_up": (LAYERS, D, FF), "w_down": (LAYERS, FF, D)}


def bump(key, n, height):
    away = (jnp.arange(n, dtype=jnp.int32) - jax.random.randint(key, (), 0, n, jnp.int32)) % n
    return jnp.where(away < n // 8, height, 1.0)


def together(key, own, strength):
    shared = jax.random.normal(key, own.shape[1:], jnp.float32)
    return (own + strength * shared) * lax.rsqrt(1 + strength * strength)


def setup_inputs(seed: int = 0, part: int = 0) -> dict:
    kx, kdy, ka, kb, kz, kf, kh, kl, *keys = jax.random.split(jax.random.key(seed), 8 + 3 * len(NAMES))
    kx, kdy, ka, kb = (jax.random.fold_in(k, part) for k in (kx, kdy, ka, kb))
    kw, km, kv = (keys[i::3] for i in range(3))
    shape = (SEQUENCES, TOKENS, D)
    much_x, much_dy = jax.random.uniform(kz, (2,), jnp.float32, 0.0, 1.0)
    loud = 2.0 ** jax.random.uniform(jax.random.fold_in(kz, 1), (), jnp.float32, -1.0, 2.0)
    layers = 2.0 ** jax.random.uniform(kl, (LAYERS, 1, 1), jnp.float32, -1.0, 1.0)
    x = together(ka, jax.random.normal(kx, shape, jnp.float32), much_x) * bump(kf, D, 4.0)
    dy = together(kb, jax.random.normal(kdy, shape, jnp.float32), much_dy)
    drawn = {"x": x.astype(jnp.bfloat16), "dy": (loud * dy * (SEQUENCES * TOKENS) ** -0.5).astype(jnp.bfloat16)}
    for key, name in zip(kw, NAMES, strict=True):
        w = jax.random.normal(key, SHAPES[name], jnp.float32) * SHAPES[name][1] ** -0.5
        drawn[name] = (w * {"w_gate": 1.0, "w_up": bump(kh, FF, 4.0), "w_down": layers}[name]).astype(jnp.bfloat16)
    for key, name in zip(km, NAMES, strict=True):
        drawn[f"m_{name}"] = 0.1 * jax.random.normal(key, SHAPES[name], jnp.float32)
    for key, name in zip(kv, NAMES, strict=True):
        drawn[f"v_{name}"] = jax.random.uniform(key, SHAPES[name], jnp.float32, 0.005, 0.015)
    return drawn


def matmul(a, w):
    return jnp.dot(a, w, preferred_element_type=jnp.float32).astype(jnp.bfloat16)


def normed(h):
    wide = h.astype(jnp.float32)
    scale = lax.rsqrt(jnp.mean(wide**2, -1, keepdims=True) + 1e-6)
    return (wide * scale).astype(jnp.bfloat16)


def layer(h, w):
    a = normed(h)
    gate = jnp.dot(a, w["w_gate"], preferred_element_type=jnp.float32)
    up = jnp.dot(a, w["w_up"], preferred_element_type=jnp.float32)
    return h + matmul((jax.nn.silu(gate) * up).astype(jnp.bfloat16), w["w_down"])


def adamw(w, m, v, g):
    m = 0.9 * m + 0.1 * g
    v = 0.95 * v + 0.05 * g * g
    step = m * lax.rsqrt(v + 1e-8) + 0.1 * w
    return (w - 0.02 * step).astype(jnp.bfloat16), m, v


def clipped(gradients, sum_of_squares, count):
    factor = jnp.minimum(1.0, 0.5 * lax.rsqrt(sum_of_squares / count + 1e-30))
    return [g * factor for g in gradients]


def stack(weights, h):
    return lax.scan(lambda h, w: (layer(h, w), None), h, weights)[0]


def reference(x, dy, w_gate, w_up, w_down, m_w_gate, m_w_up, m_w_down, v_w_gate, v_w_up, v_w_down):
    weights = dict(zip(NAMES, (w_gate, w_up, w_down), strict=True))

    def take(so_far, sequence):
        h, by_y = sequence
        _, back = jax.vjp(lambda w: stack(w, h), weights)
        return jax.tree.map(lambda total, term: total + term.astype(jnp.float32), so_far, back(by_y)[0]), None

    none_yet = {name: jnp.zeros(w.shape, jnp.float32) for name, w in weights.items()}
    by_weights, _ = lax.scan(take, none_yet, (x, dy))
    gradients = [by_weights[name].astype(jnp.bfloat16).astype(jnp.float32) for name in NAMES]
    gradients = clipped(gradients, sum(jnp.sum(g * g) for g in gradients), sum(g.size for g in gradients))
    new = [
        adamw(w.astype(jnp.float32), m, v, g)
        for w, m, v, g in zip((w_gate, w_up, w_down), (m_w_gate, m_w_up, m_w_down), (v_w_gate, v_w_up, v_w_down), gradients, strict=True)
    ]
    return tuple(one[which] for which in range(3) for one in new)
```

```python
import functools

import jax
import jax.numpy as jnp
from jax import lax
from jax.experimental import pallas as pl
from jax.experimental.pallas import tpu as pltpu
from jax.sharding import PartitionSpec as P


F32, BF16 = jnp.float32, jnp.bfloat16
T, D, FF, DP, CORES = 2048, 1024, 2816, 4, 2
COUNT = 3 * 2 * D * FF
CHUNK = 256
CHUNKS = FF // CHUNK
ROWS = 512
VMEM_LIMIT = 62 * 2**20
ANY = pl.BlockSpec(memory_space=pl.ANY)


def dot(a, b):
    return lax.dot_general(a, b, (((1,), (0,)), ((), ())), preferred_element_type=F32)


def dot_t(a, b):
    return lax.dot_general(a, b, (((1,), (1,)), ((), ())), preferred_element_type=F32)


def whole(shape):
    return pl.BlockSpec(shape, lambda *_: (0,) * len(shape), pipeline_mode=pl.Buffered(1))


def params():
    return pltpu.CompilerParams(vmem_limit_bytes=VMEM_LIMIT, dimension_semantics=("arbitrary",))


def cost(matmuls, moved):
    return pl.CostEstimate(flops=int(2 * T * D * FF * matmuls), bytes_accessed=int(moved), transcendentals=0)


def root_mean_scale(wide):
    return lax.rsqrt(jnp.mean(wide * wide, -1, keepdims=True) + 1e-6)


def forward_first(x, w_gate, w_up, w_down):
    def kernel(x_ref, wg_ref, wu_ref, wd_ref, g_ref, u_ref, a_ref, h_ref, n_ref, acc):
        j = pl.program_id(0)

        @pl.when(j == 0)
        def _():
            for t in range(0, T, ROWS):
                rows = slice(t, t + ROWS)
                wide = x_ref[rows].astype(F32)
                a_ref[rows] = (wide * root_mean_scale(wide)).astype(BF16)
                acc[rows] = jnp.zeros((ROWS, D), F32)

        for t in range(0, T, ROWS):
            rows = slice(t, t + ROWS)
            a = a_ref[rows]
            g = dot(a, wg_ref[...])
            u = dot(a, wu_ref[...])
            g_ref[rows] = g
            u_ref[rows] = u
            act = (g * jax.nn.sigmoid(g) * u).astype(BF16)
            acc[rows] += dot(act, wd_ref[...])

        @pl.when(j == CHUNKS - 1)
        def _():
            for t in range(0, T, ROWS):
                rows = slice(t, t + ROWS)
                h = x_ref[rows] + acc[rows].astype(BF16)
                h_ref[rows] = h
                wide = h.astype(F32)
                n_ref[rows] = (wide * root_mean_scale(wide)).astype(BF16)

    tall = jax.ShapeDtypeStruct((T, FF), F32)
    flat = jax.ShapeDtypeStruct((T, D), BF16)
    wide_block = pl.BlockSpec((T, CHUNK), lambda j: (0, j))
    return pl.pallas_call(
        kernel,
        grid=(CHUNKS,),
        in_specs=[
            whole((T, D)),
            pl.BlockSpec((None, D, CHUNK), lambda j: (0, 0, j)),
            pl.BlockSpec((None, D, CHUNK), lambda j: (0, 0, j)),
            pl.BlockSpec((None, CHUNK, D), lambda j: (0, j, 0)),
        ],
        out_specs=[wide_block, wide_block, whole((T, D)), whole((T, D)), whole((T, D))],
        out_shape=[tall, tall, flat, flat, flat],
        scratch_shapes=[pltpu.VMEM((T, D), F32)],
        compiler_params=params(),
        cost_estimate=cost(3, 90e6),
    )(x, w_gate, w_up, w_down)


def hidden(layer, first, count, order, normed, by_out, weights, gate_up, chain, after):
    w_gate, w_up, w_down = weights
    computed = gate_up is None
    n_chain = len(chain)
    n_after = len(after)

    def kernel(order_ref, n_ref, by_ref, wd_ref, a_ref, b_ref, *rest):
        rest = rest[n_chain + n_after :]
        if computed:
            send_ref, keep_ref, act_ref, dg_ref, du_ref, n_t, act = rest
        else:
            send_ref, keep_ref, act_ref, n_t, act, dg_ref, du_ref = rest

        @pl.when(pl.program_id(0) == 0)
        def _():
            for k in range(DP):
                columns = pl.ds(pl.multiple_of(order_ref[k] * (D // DP), D // DP), D // DP)
                n_t[k * (D // DP) : (k + 1) * (D // DP)] = n_ref[:, columns].T

        for t in range(0, T, ROWS):
            rows = slice(t, t + ROWS)
            if computed:
                n = n_ref[rows]
                g, u = dot(n, a_ref[...]), dot(n, b_ref[...])
            else:
                g, u = a_ref[rows], b_ref[rows]
            p = dot_t(by_ref[rows], wd_ref[...]).astype(BF16).astype(F32)
            sig = jax.nn.sigmoid(g)
            silu = g * sig
            act[rows] = (silu * u).astype(BF16)
            du_ref[rows] = (p * silu).astype(BF16)
            dg_ref[rows] = (p * u * (sig + silu * (1.0 - sig))).astype(BF16)
        act_ref[...] = act[...].T
        for which, d_ref in ((0, dg_ref), (1, du_ref)):
            d = d_ref[...]
            half = D // CORES
            out = dot(n_t[:half], d).astype(BF16)
            send_ref[which] = out.reshape(CORES, half // CORES, CHUNK)
            out = dot(n_t[half:], d).astype(BF16)
            keep_ref[which] = out.reshape(CORES, half // CORES, CHUNK)

    column = pl.BlockSpec((None, D, CHUNK), lambda j, _: (layer, 0, first + j))
    block = pl.BlockSpec((T, CHUNK), lambda j, _: (0, first + j))
    part = pl.BlockSpec((2, CORES, D // DP, CHUNK), lambda j, _: (0, 0, 0, j))
    part_shape = jax.ShapeDtypeStruct((2, CORES, D // DP, count * CHUNK), BF16)
    turned = pl.BlockSpec((CHUNK, T), lambda j, _: (first + j, 0))
    turned_shape = jax.ShapeDtypeStruct((FF, T), BF16)
    out_specs, out_shape = [part, part, turned], [part_shape, part_shape, turned_shape]
    scratch = [pltpu.VMEM((D, T), BF16), pltpu.VMEM((T, CHUNK), BF16)]
    if computed:
        out_specs += [block, block]
        out_shape += [jax.ShapeDtypeStruct((T, FF), BF16)] * 2
    else:
        scratch += [pltpu.VMEM((T, CHUNK), BF16)] * 2
    return pl.pallas_call(
        kernel,
        grid_spec=pltpu.PrefetchScalarGridSpec(
            num_scalar_prefetch=1,
            grid=(count,),
            in_specs=[
                whole((T, D)),
                whole((T, D)),
                pl.BlockSpec((None, CHUNK, D), lambda j, _: (layer, first + j, 0)),
                *((column, column) if computed else (block, block)),
                *(ANY,) * (n_chain + n_after),
            ],
            out_specs=out_specs,
            scratch_shapes=scratch,
        ),
        out_shape=out_shape,
        input_output_aliases={6 + i: 2 + i for i in range(n_chain)},
        compiler_params=params(),
        cost_estimate=cost((5 if computed else 3) * count / CHUNKS, 60e6 * count / CHUNKS),
    )(order, normed, by_out, w_down, *((w_gate, w_up) if computed else gate_up), *chain, *after)


def down_grad(order, act_t, by_out, first, count, after):
    n_after = len(after)

    def kernel(order_ref, send_act, keep_act, by_ref, *rest):
        send_ref, keep_ref = rest[n_after:]
        send_ref[...] = dot(send_act[...], by_ref[...]).astype(BF16)
        keep_ref[...] = dot(keep_act[...], by_ref[...]).astype(BF16)

    rows = FF // DP
    part = pl.BlockSpec((None, rows, count), lambda i, _: (i, 0, 0))
    shape = jax.ShapeDtypeStruct((CORES, rows, count), BF16)
    return pl.pallas_call(
        kernel,
        grid_spec=pltpu.PrefetchScalarGridSpec(
            num_scalar_prefetch=1,
            grid=(CORES,),
            in_specs=[
                pl.BlockSpec((rows, T), lambda i, order_ref: (order_ref[i], 0)),
                pl.BlockSpec((rows, T), lambda i, order_ref: (order_ref[CORES + i], 0)),
                pl.BlockSpec((T, count), lambda *_: (0, first // count), pipeline_mode=pl.Buffered(1)),
                *(ANY,) * n_after,
            ],
            out_specs=[part, part],
        ),
        out_shape=[shape, shape],
        compiler_params=params(),
        cost_estimate=cost(count / D, 20e6),
    )(order, act_t, act_t, by_out, *after)


def into_states(dg, du, w_gate, w_up, h, by_out, after):
    tile = 256
    n_after = len(after)

    def kernel(dg_ref, du_ref, wg_ref, wu_ref, h_ref, by_ref, *rest):
        out_ref = rest[n_after]
        by_a = dot_t(dg_ref[...], wg_ref[...]).astype(BF16) + dot_t(du_ref[...], wu_ref[...]).astype(BF16)
        c, wide = by_a.astype(F32), h_ref[...].astype(F32)
        scale = root_mean_scale(wide)
        along = jnp.sum(c * wide, -1, keepdims=True)
        out_ref[...] = by_ref[...] + (c * scale - wide * (scale * scale * scale * along * (1.0 / D))).astype(BF16)

    long = pl.BlockSpec((tile, FF), lambda i: (i, 0))
    short = pl.BlockSpec((tile, D), lambda i: (i, 0))
    weight = pl.BlockSpec((None, D, FF), lambda i: (1, 0, 0), pipeline_mode=pl.Buffered(1))
    return pl.pallas_call(
        kernel,
        grid=(T // tile,),
        in_specs=[long, long, weight, weight, short, short, *(ANY,) * n_after],
        out_specs=short,
        out_shape=jax.ShapeDtypeStruct((T, D), BF16),
        compiler_params=params(),
        cost_estimate=cost(2, 50e6),
    )(dg, du, w_gate, w_up, h, by_out, *after)


def solution(mesh):
    sibling = [(i, i ^ 1) for i in range(DP)]
    across = [(i, i ^ 2) for i in range(DP)]

    def step(x, dy, w_gate, w_up, w_down, m_gate, m_up, m_down, v_gate, v_up, v_down):
        x, dy = x[0], dy[0]
        me = lax.axis_index("dp")
        chip, core = me // CORES, me % CORES
        far, near = (1 - chip) * CORES, chip * CORES
        order = jnp.stack([far + 1 - core, near + 1 - core, far + core, near + core]).astype(jnp.int32)
        weights = (w_gate, w_up, w_down)

        def meet(send, keep, axis):
            got = lax.ppermute(send, "dp", sibling)
            pick = functools.partial(lax.index_in_dim, axis=axis, keepdims=False)
            there = (pick(keep, 0).astype(F32) + pick(got, 0).astype(F32)).astype(BF16)
            landed = lax.ppermute(there, "dp", across)
            return there, (pick(keep, 1), pick(got, 1), landed)

        def total(terms):
            one, two, three = (t.astype(F32) for t in terms)
            return (one + two + three).astype(BF16)

        g1, u1, a1, h1, a2 = forward_first(x, *weights)
        units, after, chain = {}, (), ()
        for name, first, count in (("b0", 0, 3), ("b1", 3, 4), ("b2", 7, 4)):
            send, keep, *chain = hidden(1, first, count, order, a2, dy, weights, None, chain, after)
            there, units[name] = meet(send, keep, 1)
            after = (there,)
        act2, dg2, du2 = chain
        send, keep = down_grad(order, act2, dy, 0, D, after)
        there, units["d2"] = meet(send, keep, 0)
        dh1 = into_states(dg2, du2, w_gate, w_up, h1, dy, (send,))
        after, chain = (there,), ()
        for name, first, count in (("e0", 0, 5), ("e1", 5, 6)):
            send, keep, *chain = hidden(0, first, count, order, a1, dh1, weights, (g1, u1), chain, after)
            there, units[name] = meet(send, keep, 1)
            after = (there,)
        (act1,) = chain
        for name, first in (("f0", 0), ("f1", D // 2)):
            send, keep = down_grad(order, act1, dh1, first, D // 2, after)
            there, units[name] = meet(send, keep, 0)
            after = (there,)

        grads = {name: total(terms) for name, terms in units.items()}
        squares = sum(jnp.sum(g.astype(F32) ** 2) for g in grads.values())
        squares = lax.psum(squares, "dp")
        factor = jnp.minimum(1.0, 0.5 * lax.rsqrt(squares / COUNT + 1e-30))

        def joined(which):
            if which == 2:
                return jnp.stack([jnp.concatenate([grads["f0"], grads["f1"]], 1), grads["d2"]])
            first = jnp.concatenate([grads[n][which] for n in ("e0", "e1")], 1)
            second = jnp.concatenate([grads[n][which] for n in ("b0", "b1", "b2")], 1)
            return jnp.stack([first, second])

        new_w, new_m, new_v = [], [], []
        for which, (w, m, v) in enumerate(zip(weights, (m_gate, m_up, m_down), (v_gate, v_up, v_down), strict=True)):
            rows = w.shape[1] // DP
            full = jnp.zeros(w.shape, BF16)
            g = joined(which).astype(F32) * factor
            m = 0.9 * m + 0.1 * g
            v = 0.95 * v + 0.05 * g * g
            own = lax.dynamic_slice_in_dim(w, me * rows, rows, 1).astype(F32)
            own = (own - 0.02 * (m * lax.rsqrt(v + 1e-8) + 0.1 * own)).astype(BF16)
            new_m.append(m)
            new_v.append(v)
            for layer in range(2):
                mine = own[layer : layer + 1]
                over = lax.ppermute(mine, "dp", across)
                beside = lax.ppermute(mine, "dp", sibling)
                corner = lax.ppermute(over, "dp", sibling)
                for piece, who in ((mine, me), (beside, me ^ 1), (over, me ^ 2), (corner, me ^ 3)):
                    full = lax.dynamic_update_slice(full, piece, (layer, who * rows, 0))
            new_w.append(full)
        return (*new_w, *new_m, *new_v)

    batch, replicated, rows = P(("rep", "dp"), None, None), P(None, None, None), P(None, "dp", None)
    return jax.shard_map(
        step,
        mesh=mesh,
        in_specs=(batch, batch, *(replicated,) * 3, *(rows,) * 6),
        out_specs=(*(P("rep", None, None),) * 3, *(P("rep", "dp", None),) * 6),
        check_vma=False,
    )
```

```python
import jax
import jax.numpy as jnp
from jax import lax
from jax.experimental import pallas as pl
from jax.experimental.pallas import tpu as pltpu
from jax.sharding import PartitionSpec as P


F32, BF16 = jnp.float32, jnp.bfloat16
T, D, FF, DP, CORES = 2048, 1024, 2816, 4, 2
COUNT = 3 * 2 * D * FF
CHUNK = 256
CHUNKS = FF // CHUNK
ROWS = 512
VMEM_LIMIT = 62 * 2**20
ANY = pl.BlockSpec(memory_space=pl.ANY)
MESH = pl.DeviceIdType.MESH


def dot(a, b):
    return lax.dot_general(a, b, (((1,), (0,)), ((), ())), preferred_element_type=F32)


def dot_t(a, b):
    return lax.dot_general(a, b, (((1,), (1,)), ((), ())), preferred_element_type=F32)


def whole(shape):
    return pl.BlockSpec(shape, lambda *_: (0,) * len(shape), pipeline_mode=pl.Buffered(1))


def params():
    return pltpu.CompilerParams(vmem_limit_bytes=VMEM_LIMIT, dimension_semantics=("arbitrary",))


def cost(matmuls, moved):
    return pl.CostEstimate(flops=int(2 * T * D * FF * matmuls), bytes_accessed=int(moved), transcendentals=0)


def root_mean_scale(wide):
    return lax.rsqrt(jnp.mean(wide * wide, -1, keepdims=True) + 1e-6)


def forward_first(x, w_gate, w_up, w_down):
    piece = 128
    pieces = D // piece

    def kernel(x_ref, wg_ref, wu_ref, wd_ref, g_ref, u_ref, t_ref, h_ref, n_ref, a_ref, acc):
        j = pl.program_id(0)

        @pl.when(j == 0)
        def _():
            for t in range(0, T, ROWS):
                rows = slice(t, t + ROWS)
                wide = x_ref[rows].astype(F32)
                a_ref[rows] = (wide * root_mean_scale(wide)).astype(BF16)
                acc[rows] = jnp.zeros((ROWS, D), F32)

        k = jnp.minimum(j, pieces - 1)
        per = D // DP // piece
        source = pl.multiple_of(block_of(k // per) * (D // DP) + lax.rem(k, per) * piece, piece)
        t_ref[pl.ds(pl.multiple_of(k * piece, piece), piece)] = a_ref[:, pl.ds(source, piece)].T

        for t in range(0, T, ROWS):
            rows = slice(t, t + ROWS)
            a = a_ref[rows]
            g = dot(a, wg_ref[...])
            u = dot(a, wu_ref[...])
            g_ref[rows] = g
            u_ref[rows] = u
            act = (g * jax.nn.sigmoid(g) * u).astype(BF16)
            acc[rows] += dot(act, wd_ref[...])

        @pl.when(j == CHUNKS - 1)
        def _():
            for t in range(0, T, ROWS):
                rows = slice(t, t + ROWS)
                h = x_ref[rows] + acc[rows].astype(BF16)
                h_ref[rows] = h
                wide = h.astype(F32)
                n_ref[rows] = (wide * root_mean_scale(wide)).astype(BF16)

    tall = jax.ShapeDtypeStruct((T, FF), F32)
    flat = jax.ShapeDtypeStruct((T, D), BF16)
    wide_block = pl.BlockSpec((T, CHUNK), lambda j: (0, j))
    return pl.pallas_call(
        kernel,
        grid=(CHUNKS,),
        in_specs=[
            whole((T, D)),
            pl.BlockSpec((None, D, CHUNK), lambda j: (0, 0, j)),
            pl.BlockSpec((None, D, CHUNK), lambda j: (0, 0, j)),
            pl.BlockSpec((None, CHUNK, D), lambda j: (0, j, 0)),
        ],
        out_specs=[wide_block, wide_block, whole((D, T)), whole((T, D)), whole((T, D))],
        out_shape=[tall, tall, jax.ShapeDtypeStruct((D, T), BF16), flat, flat],
        scratch_shapes=[pltpu.VMEM((T, D), BF16), pltpu.VMEM((T, D), F32)],
        compiler_params=params(),
        cost_estimate=cost(3, 90e6),
    )(x, w_gate, w_up, w_down)


def peers():
    me = lax.axis_index("dp")
    core = lax.rem(me, CORES)
    chip = me // CORES
    return chip, core, me + 1 - 2 * core, me + CORES - 2 * CORES * chip


def greet(*others):
    barrier = pltpu.get_barrier_semaphore()
    for other in others:
        pl.semaphore_signal(barrier, inc=1, device_id={"dp": other}, device_id_type=MESH)
    pl.semaphore_wait(barrier, len(others))


def block_of(i):
    chip, core, *_ = peers()
    side = lax.rem(i, CORES)
    return (side * chip + (1 - side) * (1 - chip)) * CORES + jnp.where(i < CORES, 1 - core, core)


def remote_params(ident):
    return pltpu.CompilerParams(
        vmem_limit_bytes=VMEM_LIMIT, dimension_semantics=("arbitrary",), collective_id=ident, has_side_effects=True
    )


def remote(source, landing, send_sem, recv_sem, to):
    return pltpu.make_async_remote_copy(
        src_ref=source, dst_ref=landing, send_sem=send_sem, recv_sem=recv_sem, device_id={"dp": to}, device_id_type=MESH
    )


def hidden(ident, layer, inside, lag, normed, by_out, weights, gate_up, after):
    w_gate, w_up, w_down = weights
    computed = gate_up is None
    n_after = len(after)
    rows_w = D // DP
    outside = CHUNKS - inside

    def kernel(n_ref, by_ref, wd_ref, a_ref, b_ref, *rest):
        rest = rest[n_after:]
        sum_ref, far_ref, near_ref, act_ref, *rest = rest
        if computed:
            dg_ref, du_ref, n_t, *rest = rest
        else:
            n_t = n_ref
        act, out, keep, got, far, near, landed, send_sem, recv_sem, over_send, over_recv, *rest = rest
        if not computed:
            dg_ref, du_ref = rest
        j = pl.program_id(0)
        _, _, sib, opposite = peers()

        def beside(k):
            slot = lax.rem(k, 2)
            return remote(out.at[slot], got.at[k], send_sem.at[k], recv_sem.at[k], sib)

        def over(k):
            return remote(far.at[k], landed.at[k], over_send.at[k], over_recv.at[k], opposite)

        def add(k):
            mine = keep.at[lax.rem(k, 2)]

            def sums(which):
                there = (mine[which, 0].astype(F32) + got[k, which, 0].astype(F32)).astype(BF16)
                return there, mine[which, 1].astype(F32) + got[k, which, 1].astype(F32)

            @pl.when(k < inside)
            def _():
                for which in range(2):
                    far[k, which], near[k, which] = sums(which)

            @pl.when(k >= inside)
            def _():
                columns = pl.ds(pl.multiple_of((k - inside) * CHUNK, CHUNK), CHUNK)
                for which in range(2):
                    far_ref[which, :, columns], near_ref[which, :, columns] = sums(which)

        def finish(k):
            over(k).wait()
            columns = pl.ds(pl.multiple_of(k * CHUNK, CHUNK), CHUNK)
            for which in range(2):
                sum_ref[which, :, columns] = (near[k, which] + landed[k, which].astype(F32)).astype(BF16)

        @pl.when(j == 0)
        def _():
            greet(sib, opposite)
            if computed:
                for k in range(DP):
                    columns = pl.ds(pl.multiple_of(block_of(k) * rows_w, rows_w), rows_w)
                    n_t[k * rows_w : (k + 1) * rows_w] = n_ref[:, columns].T

        for t in range(0, T, ROWS):
            rows = slice(t, t + ROWS)
            if computed:
                n = n_ref[rows]
                g, u = dot(n, a_ref[...]), dot(n, b_ref[...])
            else:
                g, u = a_ref[rows], b_ref[rows]
            p = dot_t(by_ref[rows], wd_ref[...]).astype(BF16).astype(F32)
            sig = jax.nn.sigmoid(g)
            silu = g * sig
            act[rows] = (silu * u).astype(BF16)
            du_ref[rows] = (p * silu).astype(BF16)
            dg_ref[rows] = (p * u * (sig + silu * (1.0 - sig))).astype(BF16)

        @pl.when(j > 0)
        def _():
            beside(j - 1).wait()
            add(j - 1)

        act_ref[...] = act[...].T
        half = D // CORES
        for which, d_ref in ((0, dg_ref), (1, du_ref)):
            out[lax.rem(j, 2), which] = dot(n_t[:half], d_ref[...]).astype(BF16).reshape(CORES, rows_w, CHUNK)
        for which, d_ref in ((0, dg_ref), (1, du_ref)):
            keep[lax.rem(j, 2), which] = dot(n_t[half:], d_ref[...]).astype(BF16).reshape(CORES, rows_w, CHUNK)
        beside(j).start()

        @pl.when((j > 0) & (j <= inside))
        def _():
            over(j - 1).start()

        @pl.when((j >= lag) & (j < lag + inside))
        def _():
            finish(j - lag)

        @pl.when(j == CHUNKS - 1)
        def _():
            beside(j).wait()
            add(j)
            for k in range(CHUNKS - lag, inside):
                finish(k)

    column = pl.BlockSpec((None, D, CHUNK), lambda j: (layer, 0, j))
    block = pl.BlockSpec((T, CHUNK), lambda j: (0, j))
    inner, outer = (2, rows_w, inside * CHUNK), (2, rows_w, outside * CHUNK)
    turned = pl.BlockSpec((CHUNK, T), lambda j: (j, 0))
    out_specs = [whole(inner), whole(outer), whole(outer), turned]
    out_shape = [(inner, BF16), (outer, BF16), (outer, F32), ((FF, T), BF16)]
    part, block_part = (2, CORES, rows_w, CHUNK), (inside, 2, rows_w, CHUNK)
    scratch = [
        pltpu.VMEM((T, CHUNK), BF16),
        pltpu.VMEM((2, *part), BF16),
        pltpu.VMEM((2, *part), BF16),
        pltpu.VMEM((CHUNKS, *part), BF16),
        pltpu.VMEM(block_part, BF16),
        pltpu.VMEM(block_part, F32),
        pltpu.VMEM(block_part, BF16),
        *(pltpu.SemaphoreType.DMA((CHUNKS,)),) * 2,
        *(pltpu.SemaphoreType.DMA((inside,)),) * 2,
    ]
    if computed:
        out_specs += [block, block]
        out_shape += [((T, FF), BF16)] * 2
        scratch = [pltpu.VMEM((D, T), BF16), *scratch]
    else:
        scratch += [pltpu.VMEM((T, CHUNK), BF16)] * 2
    return pl.pallas_call(
        kernel,
        grid=(CHUNKS,),
        in_specs=[
            whole(normed.shape),
            whole((T, D)),
            pl.BlockSpec((None, CHUNK, D), lambda j: (layer, j, 0)),
            *((column, column) if computed else (block, block)),
            *(ANY,) * n_after,
        ],
        out_specs=out_specs,
        out_shape=[jax.ShapeDtypeStruct(*one) for one in out_shape],
        scratch_shapes=scratch,
        compiler_params=remote_params(ident),
        cost_estimate=cost(5 if computed else 3, 60e6),
    )(normed, by_out, w_down, *((w_gate, w_up) if computed else gate_up), *after)


def down_grad(ident, act_t, by_out, first, count, after):
    n_after = len(after)
    rows_w = FF // DP

    def kernel(act_ref, by_ref, *rest):
        far_ref, near_ref, out, got, send_sem, recv_sem = rest[n_after:]
        i = pl.program_id(0)
        sib = peers()[2]

        def copy(k):
            return remote(out.at[k], got.at[k], send_sem.at[k], recv_sem.at[k], sib)

        pl.when(i == 0)(lambda: greet(sib))
        term = dot(act_ref[...], by_ref[...]).astype(BF16)

        @pl.when(i < CORES)
        def _():
            out[lax.rem(i, CORES)] = term

        for k in range(CORES):

            @pl.when(i == k + 1)
            def _(k=k):
                copy(k).start()

        @pl.when(i == CORES)
        def _():
            copy(0).wait()
            far_ref[...] = (term.astype(F32) + got[0].astype(F32)).astype(BF16)

        @pl.when(i == CORES + 1)
        def _():
            copy(1).wait()
            near_ref[...] = term.astype(F32) + got[1].astype(F32)

    shape = (rows_w, count)
    return pl.pallas_call(
        kernel,
        grid=(DP,),
        in_specs=[
            pl.BlockSpec((rows_w, T), lambda i: (block_of(i), 0)),
            pl.BlockSpec((T, count), lambda i: (0, first // count), pipeline_mode=pl.Buffered(1)),
            *(ANY,) * n_after,
        ],
        out_specs=[whole(shape), whole(shape)],
        out_shape=[jax.ShapeDtypeStruct(shape, BF16), jax.ShapeDtypeStruct(shape, F32)],
        scratch_shapes=[
            pltpu.VMEM((CORES, *shape), BF16),
            pltpu.VMEM((CORES, *shape), BF16),
            pltpu.SemaphoreType.DMA((CORES,)),
            pltpu.SemaphoreType.DMA((CORES,)),
        ],
        compiler_params=remote_params(ident),
        cost_estimate=cost(count / D, 20e6),
    )(act_t, by_out, *after)


def new_weight(layer, me, factor, g, m, v, w, full):
    rows, columns = g.shape
    steps = 4
    tile = rows // steps
    n_full = full is not None

    def kernel(me_ref, factor_ref, g_ref, m_ref, v_ref, w_ref, *rest):
        out_ref, full_ref = rest[n_full:]
        g = g_ref[...].astype(F32) * factor_ref[0]
        m = 0.9 * m_ref[...] + 0.1 * g
        v = 0.95 * v_ref[...] + 0.05 * g * g
        w = w_ref[...].astype(F32)
        new = (w - 0.02 * (m * lax.rsqrt(v + 1e-8) + 0.1 * w)).astype(BF16)
        out_ref[...] = new
        full_ref[...] = new

    mine = pl.BlockSpec((tile, columns), lambda i, _: (i, 0))
    state = pl.BlockSpec((None, tile, columns), lambda i, _: (layer, i, 0))
    own = pl.BlockSpec((None, tile, columns), lambda i, me_ref: (layer, me_ref[0] * steps + i, 0))
    return pl.pallas_call(
        kernel,
        grid_spec=pltpu.PrefetchScalarGridSpec(
            num_scalar_prefetch=1,
            grid=(steps,),
            in_specs=[pl.BlockSpec(memory_space=pltpu.SMEM), mine, state, state, own, *(ANY,) * n_full],
            out_specs=[mine, own],
        ),
        out_shape=[jax.ShapeDtypeStruct((rows, columns), BF16), jax.ShapeDtypeStruct(w.shape, BF16)],
        input_output_aliases={6: 1} if n_full else {},
        compiler_params=params(),
        cost_estimate=cost(0.1, 10e6),
    )(me.reshape(1), factor.reshape(1), g, m, v, w, *((full,) if n_full else ()))


def into_states(dg, du, w_gate, w_up, h, by_out, after):
    tile = 256
    n_after = len(after)

    def kernel(dg_ref, du_ref, wg_ref, wu_ref, h_ref, by_ref, *rest):
        out_ref = rest[n_after]
        by_a = dot_t(dg_ref[...], wg_ref[...]).astype(BF16) + dot_t(du_ref[...], wu_ref[...]).astype(BF16)
        c, wide = by_a.astype(F32), h_ref[...].astype(F32)
        scale = root_mean_scale(wide)
        along = jnp.sum(c * wide, -1, keepdims=True)
        out_ref[...] = by_ref[...] + (c * scale - wide * (scale * scale * scale * along * (1.0 / D))).astype(BF16)

    long = pl.BlockSpec((tile, FF), lambda i: (i, 0))
    short = pl.BlockSpec((tile, D), lambda i: (i, 0))
    weight = pl.BlockSpec((None, D, FF), lambda i: (1, 0, 0), pipeline_mode=pl.Buffered(1))
    return pl.pallas_call(
        kernel,
        grid=(T // tile,),
        in_specs=[long, long, weight, weight, short, short, *(ANY,) * n_after],
        out_specs=short,
        out_shape=jax.ShapeDtypeStruct((T, D), BF16),
        compiler_params=params(),
        cost_estimate=cost(2, 50e6),
    )(dg, du, w_gate, w_up, h, by_out, *after)


def solution(mesh):
    sibling = [(i, i ^ 1) for i in range(DP)]
    across = [(i, i ^ 2) for i in range(DP)]

    def step(x, dy, w_gate, w_up, w_down, m_gate, m_up, m_down, v_gate, v_up, v_down):
        x, dy = x[0], dy[0]
        me = lax.axis_index("dp")
        weights = (w_gate, w_up, w_down)

        def cross(far):
            return lax.ppermute(far, "dp", across)

        g1, u1, a1, h1, a2 = forward_first(x, *weights)
        units = {}
        sum_b, far, near, act2, dg2, du2 = hidden(0, 1, 9, 3, a2, dy, weights, None, ())
        units["b"] = near, cross(far)
        far, near = down_grad(1, act2, dy, 0, D, (far,))
        units["d"] = near, cross(far)
        dh1 = into_states(dg2, du2, w_gate, w_up, h1, dy, (far,))
        sum_e, far, near, act1 = hidden(2, 0, 7, 5, a1, dh1, weights, (g1, u1), ())
        units["e"] = near, cross(far)
        far, near = down_grad(3, act1, dh1, 0, D, (far,))
        units["f"] = near, cross(far)

        nears = {name: near for name, (near, _) in units.items()}
        nears, sum_b, sum_e, _ = lax.optimization_barrier((nears, sum_b, sum_e, far))
        units = {name: (nears[name], landed) for name, (_, landed) in units.items()}
        grads, squared = {}, []
        for name, (near, landed) in units.items():
            grads[name] = (near + landed.astype(F32)).astype(BF16)
            squared.append(jnp.sum(grads[name].astype(F32) ** 2))
            if name in "be":
                inner = sum_b if name == "b" else sum_e
                squared.append(jnp.sum(inner.astype(F32) ** 2))
                grads[name] = jnp.concatenate([inner, grads[name]], 2)

        def of(which, layer):
            if which == 2:
                return grads["d" if layer else "f"]
            return grads["b" if layer else "e"][which]

        each = {(which, layer): of(which, layer) for which in range(3) for layer in range(2)}
        squares, each = lax.optimization_barrier((sum(squared), each))
        squares = lax.psum(squares, "dp")
        factor = jnp.minimum(1.0, 0.5 * lax.rsqrt(squares / COUNT + 1e-30))

        ms, vs = (m_gate, m_up, m_down), (v_gate, v_up, v_down)
        full, sent = [None] * 3, []
        for (which, layer), g in each.items():
            name = f"{which}{layer}"
            mine, full[which] = new_weight(layer, me, factor, g, ms[which], vs[which], weights[which], full[which])
            over = lax.ppermute(mine, "dp", across)
            beside = lax.ppermute(mine, "dp", sibling)
            sent.append((which, layer, over, beside))
        factor, _ = lax.optimization_barrier((factor, mine))
        new_m, new_v = [], []
        for which in range(3):
            g = jnp.stack([each[which, 0], each[which, 1]]).astype(F32) * factor
            new_m.append(0.9 * ms[which] + 0.1 * g)
            new_v.append(0.95 * vs[which] + 0.05 * g * g)
        for k, (which, layer, over, beside) in enumerate(sent):
            if 1 <= k <= 3:
                full, new_m[k - 1], new_v[k - 1] = lax.optimization_barrier((full, new_m[k - 1], new_v[k - 1]))
            over, beside, full = lax.optimization_barrier((over, beside, full))
            corner = lax.ppermute(over, "dp", sibling)
            for piece, who in ((beside, me ^ 1), (over, me ^ 2), (corner, me ^ 3)):
                full[which] = lax.dynamic_update_slice(full[which], piece[None], (layer, who * piece.shape[0], 0))
        return (*full, *new_m, *new_v)

    batch, replicated, rows = P(("rep", "dp"), None, None), P(None, None, None), P(None, "dp", None)
    return jax.shard_map(
        step,
        mesh=mesh,
        in_specs=(batch, batch, *(replicated,) * 3, *(rows,) * 6),
        out_specs=(*(P("rep", None, None),) * 3, *(P("rep", "dp", None),) * 6),
        check_vma=False,
    )
```

```python
import jax
import jax.numpy as jnp
from jax import lax
from jax.experimental import pallas as pl
from jax.experimental.pallas import tpu as pltpu
from jax.sharding import PartitionSpec as P


F32, BF16 = jnp.float32, jnp.bfloat16
T, D, FF, DP, CORES = 2048, 1024, 2816, 4, 2
COUNT = 3 * 2 * D * FF
CHUNK = 256
CHUNKS = FF // CHUNK
ROWS = 512
TILE = 256
VMEM_LIMIT = 62 * 2**20
ANY = pl.BlockSpec(memory_space=pl.ANY)
MESH = pl.DeviceIdType.MESH


def dot(a, b):
    return lax.dot_general(a, b, (((1,), (0,)), ((), ())), preferred_element_type=F32)


def dot_t(a, b):
    return lax.dot_general(a, b, (((1,), (1,)), ((), ())), preferred_element_type=F32)


def whole(shape):
    return pl.BlockSpec(shape, lambda *_: (0,) * len(shape), pipeline_mode=pl.Buffered(1))


def params():
    return pltpu.CompilerParams(vmem_limit_bytes=VMEM_LIMIT, dimension_semantics=("arbitrary",))


def cost(matmuls, moved):
    return pl.CostEstimate(flops=int(2 * T * D * FF * matmuls), bytes_accessed=int(moved), transcendentals=0)


def root_mean_scale(wide):
    return lax.rsqrt(jnp.mean(wide * wide, -1, keepdims=True) + 1e-6)


def forward_first(x, w_gate, w_up, w_down):
    piece = 128
    pieces = D // piece

    def kernel(x_ref, wg_ref, wu_ref, wd_ref, g_ref, u_ref, t_ref, h_ref, n_ref, a_ref, held_h, acc, h_sem, n_sem):
        j = pl.program_id(0)

        @pl.when(j == 0)
        def _():
            @pl.loop(0, T // TILE)
            def _(t):
                rows = pl.ds(pl.multiple_of(t * TILE, TILE), TILE)
                wide = x_ref[rows].astype(F32)
                a_ref[rows] = (wide * root_mean_scale(wide)).astype(BF16)

        k = jnp.minimum(j, pieces - 1)
        per = D // DP // piece
        source = pl.multiple_of(block_of(k // per) * (D // DP) + lax.rem(k, per) * piece, piece)
        t_ref[...] = a_ref[:, pl.ds(source, piece)].T

        for t in range(0, T, ROWS):
            rows = slice(t, t + ROWS)
            a = a_ref[rows]
            g = dot(a, wg_ref[...])
            u = dot(a, wu_ref[...])
            g_ref[rows] = g
            u_ref[rows] = u
            act = (g * jax.nn.sigmoid(g) * u).astype(BF16)
            acc[rows] = jnp.where(j > 0, acc[rows], 0.0) + dot(act, wd_ref[...])

        @pl.when(j == CHUNKS - 1)
        def _():
            def copies(t):
                rows = pl.ds(pl.multiple_of(t * TILE, TILE), TILE)
                return (
                    pltpu.make_async_copy(held_h.at[rows], h_ref.at[rows], h_sem.at[t]),
                    pltpu.make_async_copy(a_ref.at[rows], n_ref.at[rows], n_sem.at[t]),
                )

            @pl.loop(0, T // TILE)
            def _(t):
                rows = pl.ds(pl.multiple_of(t * TILE, TILE), TILE)
                h = x_ref[rows] + acc[rows].astype(BF16)
                held_h[rows] = h
                wide = h.astype(F32)
                a_ref[rows] = (wide * root_mean_scale(wide)).astype(BF16)
                for one in copies(t):
                    one.start()

            @pl.loop(0, T // TILE)
            def _(t):
                for one in copies(t):
                    one.wait()

    tall = jax.ShapeDtypeStruct((T, FF), F32)
    flat = jax.ShapeDtypeStruct((T, D), BF16)
    wide_block = pl.BlockSpec((T, CHUNK), lambda j: (0, j))
    return pl.pallas_call(
        kernel,
        grid=(CHUNKS,),
        in_specs=[
            whole((T, D)),
            pl.BlockSpec((None, D, CHUNK), lambda j: (0, 0, j)),
            pl.BlockSpec((None, D, CHUNK), lambda j: (0, 0, j)),
            pl.BlockSpec((None, CHUNK, D), lambda j: (0, j, 0)),
        ],
        out_specs=[wide_block, wide_block, pl.BlockSpec((piece, T), lambda j: (jnp.minimum(j, pieces - 1), 0)), ANY, ANY],
        out_shape=[tall, tall, jax.ShapeDtypeStruct((D, T), BF16), flat, flat],
        scratch_shapes=[
            pltpu.VMEM((T, D), BF16),
            pltpu.VMEM((T, D), BF16),
            pltpu.VMEM((T, D), F32),
            *(pltpu.SemaphoreType.DMA((T // TILE,)),) * 2,
        ],
        compiler_params=params(),
        cost_estimate=cost(3, 90e6),
    )(x, w_gate, w_up, w_down)


def peers():
    me = lax.axis_index("dp")
    core = lax.rem(me, CORES)
    chip = me // CORES
    return chip, core, me + 1 - 2 * core, me + CORES - 2 * CORES * chip


def greet(*others):
    barrier = pltpu.get_barrier_semaphore()
    for other in others:
        pl.semaphore_signal(barrier, inc=1, device_id={"dp": other}, device_id_type=MESH)
    pl.semaphore_wait(barrier, len(others))


def block_of(i):
    chip, core, *_ = peers()
    side = lax.rem(i, CORES)
    return (side * chip + (1 - side) * (1 - chip)) * CORES + jnp.where(i < CORES, 1 - core, core)


def remote_params(ident):
    return pltpu.CompilerParams(
        vmem_limit_bytes=VMEM_LIMIT, dimension_semantics=("arbitrary",), collective_id=ident, has_side_effects=True
    )


def remote(source, landing, send_sem, recv_sem, to):
    return pltpu.make_async_remote_copy(
        src_ref=source, dst_ref=landing, send_sem=send_sem, recv_sem=recv_sem, device_id={"dp": to}, device_id_type=MESH
    )


def hidden(ident, layer, inside, lag, quick, normed, by_out, weights, gate_up, after):
    w_gate, w_up, w_down = weights
    computed = gate_up is None
    n_after = len(after)
    rows_w = D // DP
    outside = CHUNKS - inside

    def kernel(n_ref, by_ref, wd_ref, a_ref, b_ref, *rest):
        rest = rest[n_after:]
        sum_ref, far_ref, near_ref, act_ref, *rest = rest
        if computed:
            dg_ref, du_ref, n_t, *rest = rest
        else:
            n_t = n_ref
        act, out, keep, got, far, near, landed, send_sem, recv_sem, over_send, over_recv, *rest = rest
        if not computed:
            dg_ref, du_ref = rest
        j = pl.program_id(0)
        _, _, sib, opposite = peers()

        def beside(k):
            slot = lax.rem(k, 2)
            return remote(out.at[slot], got.at[k], send_sem.at[k], recv_sem.at[k], sib)

        def over(k):
            return remote(far.at[k], landed.at[k], over_send.at[k], over_recv.at[k], opposite)

        def add(k, at):
            mine = keep.at[lax.rem(k + 2, 2)]
            for which in range(2):
                far[at, which] = (mine[which, 0].astype(F32) + got[at, which, 0].astype(F32)).astype(BF16)
                near[at, which] = mine[which, 1].astype(F32) + got[at, which, 1].astype(F32)

        def finish(k, at):
            columns = pl.ds(pl.multiple_of(k * CHUNK, CHUNK), CHUNK)
            for which in range(2):
                sum_ref[which, :, columns] = (near[k, which] + landed[at, which].astype(F32)).astype(BF16)

        barrier = pltpu.get_barrier_semaphore()

        @pl.when(j == 0)
        def _():
            for other in (sib, opposite):
                pl.semaphore_signal(barrier, inc=1, device_id={"dp": other}, device_id_type=MESH)
            if computed:

                @pl.loop(0, DP)
                def _(k):
                    columns = pl.ds(pl.multiple_of(block_of(k) * rows_w, rows_w), rows_w)
                    n_t[pl.ds(pl.multiple_of(k * rows_w, rows_w), rows_w)] = n_ref[:, columns].T

        if not quick:

            @pl.when(j > 1)
            def _():
                beside(j - 2).wait()

        @pl.when((j >= lag) & (j < lag + inside))
        def _():
            over(j - lag).wait()

        for t in range(0, T, ROWS):
            rows = slice(t, t + ROWS)
            if computed:
                n = n_ref[rows]
                g, u = dot(n, a_ref[...]), dot(n, b_ref[...])
            else:
                g, u = a_ref[rows], b_ref[rows]
            p = dot_t(by_ref[rows], wd_ref[...]).astype(BF16).astype(F32)
            sig = jax.nn.sigmoid(g)
            silu = g * sig
            act[rows] = (silu * u).astype(BF16)
            du_ref[rows] = (p * silu).astype(BF16)
            dg_ref[rows] = (p * u * (sig + silu * (1.0 - sig))).astype(BF16)

        if not quick:
            add(j - 2, jnp.where(j > 1, j - 2, CHUNKS))
        finish(jnp.clip(j - lag, 0, inside - 1), jnp.where(j < lag, inside, jnp.minimum(j - lag, inside - 1)))
        act_ref[...] = act[...].T
        half = D // CORES
        for which, d_ref in ((0, dg_ref), (1, du_ref)):
            out[lax.rem(j, 2), which] = dot(n_t[:half], d_ref[...]).astype(BF16).reshape(CORES, rows_w, CHUNK)
        for which, d_ref in ((0, dg_ref), (1, du_ref)):
            keep[lax.rem(j, 2), which] = dot(n_t[half:], d_ref[...]).astype(BF16).reshape(CORES, rows_w, CHUNK)

        @pl.when(j == 0)
        def _():
            pl.semaphore_wait(barrier, 2)

        beside(j).start()
        late = 1 if quick else 2

        def meet(k):
            beside(k).wait()
            add(k, k)

        if quick:

            @pl.when(j == 0)
            def _():
                meet(0)
                over(0).start()

            @pl.when(j > 1)
            def _():
                meet(j - 1)

        @pl.when((j >= 2) & (j < inside + late))
        def _():
            over(j - late).start()

        @pl.when(j == CHUNKS - 1)
        def _():
            pl.loop(CHUNKS - late, CHUNKS)(meet)

            @pl.loop(CHUNKS - lag, inside)
            def _(k):
                over(k).wait()
                finish(k, k)

            @pl.loop(inside, CHUNKS)
            def _(k):
                columns = pl.ds(pl.multiple_of((k - inside) * CHUNK, CHUNK), CHUNK)
                for which in range(2):
                    far_ref[which, :, columns], near_ref[which, :, columns] = far[k, which], near[k, which]

    column = pl.BlockSpec((None, D, CHUNK), lambda j: (layer, 0, j))
    block = pl.BlockSpec((T, CHUNK), lambda j: (0, j))
    inner, outer = (2, rows_w, inside * CHUNK), (2, rows_w, outside * CHUNK)
    turned = pl.BlockSpec((CHUNK, T), lambda j: (j, 0))
    out_specs = [whole(inner), whole(outer), whole(outer), turned]
    out_shape = [(inner, BF16), (outer, BF16), (outer, F32), ((FF, T), BF16)]
    part, block_part = (2, CORES, rows_w, CHUNK), (2, rows_w, CHUNK)
    scratch = [
        pltpu.VMEM((T, CHUNK), BF16),
        pltpu.VMEM((2, *part), BF16),
        pltpu.VMEM((2, *part), BF16),
        pltpu.VMEM((CHUNKS + 1, *part), BF16),
        pltpu.VMEM((CHUNKS + 1, *block_part), BF16),
        pltpu.VMEM((CHUNKS + 1, *block_part), F32),
        pltpu.VMEM((inside + 1, *block_part), BF16),
        *(pltpu.SemaphoreType.DMA((CHUNKS,)),) * 2,
        *(pltpu.SemaphoreType.DMA((inside,)),) * 2,
    ]
    if computed:
        out_specs += [block, block]
        out_shape += [((T, FF), BF16)] * 2
        scratch = [pltpu.VMEM((D, T), BF16), *scratch]
    else:
        scratch += [pltpu.VMEM((T, CHUNK), BF16)] * 2
    return pl.pallas_call(
        kernel,
        grid=(CHUNKS,),
        in_specs=[
            whole(normed.shape),
            whole((T, D)),
            pl.BlockSpec((None, CHUNK, D), lambda j: (layer, j, 0)),
            *((column, column) if computed else (block, block)),
            *(ANY,) * n_after,
        ],
        out_specs=out_specs,
        out_shape=[jax.ShapeDtypeStruct(*one) for one in out_shape],
        scratch_shapes=scratch,
        compiler_params=remote_params(ident),
        cost_estimate=cost(5 if computed else 3, 60e6),
    )(normed, by_out, w_down, *((w_gate, w_up) if computed else gate_up), *after)


def down_grad(ident, act_t, by_out, parts, after):
    n_after = len(after)
    rows_w = FF // DP

    def kernel(act_ref, by_ref, *rest):
        *far_refs, near_ref, out, got, send_sem, recv_sem = rest[n_after:]
        i = pl.program_id(0)
        sib = peers()[2]

        def copy(k):
            return remote(out.at[k], got.at[k], send_sem.at[k], recv_sem.at[k], sib)

        barrier = pltpu.get_barrier_semaphore()

        @pl.when(i == 0)
        def _():
            pl.semaphore_signal(barrier, inc=1, device_id={"dp": sib}, device_id_type=MESH)

        @pl.when(i == 1)
        def _():
            pl.semaphore_wait(barrier, 1)

        term = dot(act_ref[...], by_ref[...]).astype(BF16)

        @pl.when(i < CORES)
        def _():
            out[lax.rem(i, CORES)] = term

        for k in range(CORES):

            @pl.when(i == k + 1)
            def _(k=k):
                copy(k).start()

        @pl.when(i == CORES)
        def _():
            copy(0).wait()
            far = (term.astype(F32) + got[0].astype(F32)).astype(BF16)
            for k, far_ref in enumerate(far_refs):
                far_ref[...] = far[:, k * D // parts : (k + 1) * D // parts]

        @pl.when(i == CORES + 1)
        def _():
            copy(1).wait()
            near_ref[...] = term.astype(F32) + got[1].astype(F32)

    shape, far_shape = (rows_w, D), (rows_w, D // parts)
    return pl.pallas_call(
        kernel,
        grid=(DP,),
        in_specs=[
            pl.BlockSpec((rows_w, T), lambda i: (block_of(i), 0)),
            whole((T, D)),
            *(ANY,) * n_after,
        ],
        out_specs=[*(whole(far_shape),) * parts, whole(shape)],
        out_shape=[*(jax.ShapeDtypeStruct(far_shape, BF16),) * parts, jax.ShapeDtypeStruct(shape, F32)],
        scratch_shapes=[
            pltpu.VMEM((CORES, *shape), BF16),
            pltpu.VMEM((CORES, *shape), BF16),
            pltpu.SemaphoreType.DMA((CORES,)),
            pltpu.SemaphoreType.DMA((CORES,)),
        ],
        compiler_params=remote_params(ident),
        cost_estimate=cost(1, 20e6),
    )(act_t, by_out, *after)


def clip_and_first(ident, squares, g, m, v, w):
    rows, columns = g.shape
    tile = 64

    def kernel(squares_ref, g_ref, m_ref, v_ref, w_ref, factor_ref, out_ref, held_g, held_m, held_v, held_w, mine, theirs, load, send_sem, recv_sem):
        chip, core, sib, opposite = peers()
        own = pl.ds(pl.multiple_of((chip * CORES + core) * rows, rows), rows)
        loads = [
            pltpu.make_async_copy(g_ref, held_g, load.at[0]),
            pltpu.make_async_copy(m_ref.at[0], held_m, load.at[1]),
            pltpu.make_async_copy(v_ref.at[0], held_v, load.at[2]),
            pltpu.make_async_copy(w_ref.at[0, own], held_w, load.at[3]),
        ]
        for one in loads:
            one.start()
        mine[...] = jnp.full(mine.shape, squares_ref[0], F32)
        others = (sib, opposite, opposite + 1 - 2 * core)
        greet(*others)
        copies = [remote(mine, theirs.at[k], send_sem.at[k], recv_sem.at[k], other) for k, other in enumerate(others)]
        for one in copies:
            one.start()
        for one in copies:
            one.wait()
        total = (mine[...] + theirs[0]) + (theirs[1] + theirs[2])
        factor = jnp.minimum(1.0, 0.5 * lax.rsqrt(total / COUNT + 1e-30))
        factor_ref[...] = factor
        for one in loads:
            one.wait()

        @pl.loop(0, rows // tile)
        def _(t):
            at = pl.ds(pl.multiple_of(t * tile, tile), tile)
            out_ref[at] = updated(factor[:1, :1], held_g[at], held_m[at], held_v[at], held_w[at])

    return pl.pallas_call(
        kernel,
        in_specs=[pl.BlockSpec(memory_space=pltpu.SMEM), *(ANY,) * 4],
        out_specs=[pl.BlockSpec(memory_space=pltpu.VMEM)] * 2,
        out_shape=[jax.ShapeDtypeStruct((8, 128), F32), jax.ShapeDtypeStruct((rows, columns), BF16)],
        scratch_shapes=[
            pltpu.VMEM((rows, columns), BF16),
            pltpu.VMEM((rows, columns), F32),
            pltpu.VMEM((rows, columns), F32),
            pltpu.VMEM((rows, columns), BF16),
            pltpu.VMEM((8, 128), F32),
            pltpu.VMEM((DP - 1, 8, 128), F32),
            pltpu.SemaphoreType.DMA((4,)),
            pltpu.SemaphoreType.DMA((DP - 1,)),
            pltpu.SemaphoreType.DMA((DP - 1,)),
        ],
        compiler_params=pltpu.CompilerParams(vmem_limit_bytes=VMEM_LIMIT, collective_id=ident, has_side_effects=True),
        cost_estimate=cost(0.1, 10e6),
    )(squares.reshape(1), g, m, v, w)


def updated(factor, g, m, v, w):
    g = g.astype(F32) * factor
    m = 0.9 * m + 0.1 * g
    v = 0.95 * v + 0.05 * g * g
    w = w.astype(F32)
    return (w - 0.02 * (m * lax.rsqrt(v + 1e-8) + 0.1 * w)).astype(BF16)


def new_weight(layer, me, factor, g, m, v, w, full):
    rows, columns = g.shape
    steps = 4
    tile = rows // steps
    n_full = full is not None

    def kernel(me_ref, factor_ref, g_ref, m_ref, v_ref, w_ref, *rest):
        out_ref, full_ref = rest[n_full:]
        new = updated(factor_ref[:1, :1], g_ref[...], m_ref[...], v_ref[...], w_ref[...])
        out_ref[...] = new
        full_ref[...] = new

    mine = pl.BlockSpec((tile, columns), lambda i, _: (i, 0))
    state = pl.BlockSpec((None, tile, columns), lambda i, _: (layer, i, 0))
    own = pl.BlockSpec((None, tile, columns), lambda i, me_ref: (layer, me_ref[0] * steps + i, 0))
    return pl.pallas_call(
        kernel,
        grid_spec=pltpu.PrefetchScalarGridSpec(
            num_scalar_prefetch=1,
            grid=(steps,),
            in_specs=[whole((8, 128)), mine, state, state, own, *(ANY,) * n_full],
            out_specs=[mine, own],
        ),
        out_shape=[jax.ShapeDtypeStruct((rows, columns), BF16), jax.ShapeDtypeStruct(w.shape, BF16)],
        input_output_aliases={6: 1} if n_full else {},
        compiler_params=params(),
        cost_estimate=cost(0.1, 10e6),
    )(me.reshape(1), factor, g, m, v, w, *((full,) if n_full else ()))


def into_states(dg, du, w_gate, w_up, h, by_out, after):
    tile = 256
    n_after = len(after)

    def kernel(dg_ref, du_ref, wg_ref, wu_ref, h_ref, by_ref, *rest):
        out_ref = rest[n_after]
        by_a = dot_t(dg_ref[...], wg_ref[...]).astype(BF16) + dot_t(du_ref[...], wu_ref[...]).astype(BF16)
        c, wide = by_a.astype(F32), h_ref[...].astype(F32)
        scale = root_mean_scale(wide)
        along = jnp.sum(c * wide, -1, keepdims=True)
        out_ref[...] = by_ref[...] + (c * scale - wide * (scale * scale * scale * along * (1.0 / D))).astype(BF16)

    long = pl.BlockSpec((tile, FF), lambda i: (i, 0))
    short = pl.BlockSpec((tile, D), lambda i: (i, 0))
    weight = pl.BlockSpec((None, D, FF), lambda i: (1, 0, 0), pipeline_mode=pl.Buffered(1))
    return pl.pallas_call(
        kernel,
        grid=(T // tile,),
        in_specs=[long, long, weight, weight, short, short, *(ANY,) * n_after],
        out_specs=short,
        out_shape=jax.ShapeDtypeStruct((T, D), BF16),
        compiler_params=params(),
        cost_estimate=cost(2, 50e6),
    )(dg, du, w_gate, w_up, h, by_out, *after)


def solution(mesh):
    sibling = [(i, i ^ 1) for i in range(DP)]
    across = [(i, i ^ 2) for i in range(DP)]

    def step(x, dy, w_gate, w_up, w_down, m_gate, m_up, m_down, v_gate, v_up, v_down):
        x, dy = x[0], dy[0]
        me = lax.axis_index("dp")
        weights = (w_gate, w_up, w_down)

        def cross(far):
            return lax.ppermute(far, "dp", across)

        g1, u1, a1, h1, a2 = forward_first(x, *weights)
        units = {}
        sum_b, far, near, act2, dg2, du2 = hidden(0, 1, 8, 6, False, a2, dy, weights, None, ())
        units["b"] = near, cross(far)
        far, near = down_grad(1, act2, dy, 1, (far,))
        units["d"] = near, cross(far)
        dh1 = into_states(dg2, du2, w_gate, w_up, h1, dy, (far,))
        sum_e, far, near, act1 = hidden(2, 0, 7, 7, True, a1, dh1, weights, (g1, u1), ())
        units["e"] = near, cross(far)
        *fars, near = down_grad(3, act1, dh1, 2, (far,))
        for k, far in enumerate(fars):
            units[f"f{k}"] = near[:, k * D // 2 : (k + 1) * D // 2], cross(far)

        nears = {name: near for name, (near, _) in units.items()}
        nears, sum_b, sum_e, _ = lax.optimization_barrier((nears, sum_b, sum_e, fars))
        units = {name: (nears[name], landed) for name, (_, landed) in units.items()}
        grads, squared = {}, []
        for name, (near, landed) in units.items():
            grads[name] = (near + landed.astype(F32)).astype(BF16)
            squared.append(jnp.sum(grads[name].astype(F32) ** 2))
            if name in "be":
                inner = sum_b if name == "b" else sum_e
                squared.append(jnp.sum(inner.astype(F32) ** 2))
                grads[name] = jnp.concatenate([inner, grads[name]], 2)

        def of(which, layer):
            if which == 2:
                return grads["d"] if layer else jnp.concatenate([grads["f0"], grads["f1"]], 1)
            return grads["b" if layer else "e"][which]

        each = {(which, layer): of(which, layer) for which in range(3) for layer in range(2)}
        squares, each = lax.optimization_barrier((sum(squared), each))

        ms, vs = (m_gate, m_up, m_down), (v_gate, v_up, v_down)
        full, sent = [None] * 3, []
        for (which, layer), g in each.items():
            name = f"{which}{layer}"
            if not sent:
                factor, mine = clip_and_first(4, squares, g, ms[which], vs[which], weights[which])
            else:
                mine, full[which] = new_weight(layer, me, factor, g, ms[which], vs[which], weights[which], full[which])
            over = lax.ppermute(mine, "dp", across)
            beside = lax.ppermute(mine, "dp", sibling)
            sent.append((which, layer, over, beside))
            first = mine if which + layer == 0 else first
        factor, _ = lax.optimization_barrier((factor[0, 0], mine))
        new_m, new_v = [], []
        for which in range(3):
            g = jnp.stack([each[which, 0], each[which, 1]]).astype(F32) * factor
            new_m.append(0.9 * ms[which] + 0.1 * g)
            new_v.append(0.95 * vs[which] + 0.05 * g * g)
        for k, (which, layer, over, beside) in enumerate(sent):
            if 1 <= k <= 3:
                full, new_m[k - 1], new_v[k - 1] = lax.optimization_barrier((full, new_m[k - 1], new_v[k - 1]))
            over, beside, full = lax.optimization_barrier((over, beside, full))
            corner = lax.ppermute(over, "dp", sibling)
            own = ((first, me),) if k == 0 else ()
            for piece, who in (*own, (beside, me ^ 1), (over, me ^ 2), (corner, me ^ 3)):
                full[which] = lax.dynamic_update_slice(full[which], piece[None], (layer, who * piece.shape[0], 0))
        return (*full, *new_m, *new_v)

    batch, replicated, rows = P(("rep", "dp"), None, None), P(None, None, None), P(None, "dp", None)
    return jax.shard_map(
        step,
        mesh=mesh,
        in_specs=(batch, batch, *(replicated,) * 3, *(rows,) * 6),
        out_specs=(*(P("rep", None, None),) * 3, *(P("rep", "dp", None),) * 6),
        check_vma=False,
    )
```

```python
import jax
import jax.numpy as jnp
from jax import lax
from jax.experimental import pallas as pl
from jax.experimental.pallas import tpu as pltpu
from jax.sharding import PartitionSpec as P


F32, BF16 = jnp.float32, jnp.bfloat16
T, D, FF, DP, CORES = 2048, 1024, 2816, 4, 2
COUNT = 3 * 2 * D * FF
CHUNK = 256
CHUNKS = FF // CHUNK
ROWS = 512
TILE = 256
VMEM_LIMIT = 62 * 2**20
ANY = pl.BlockSpec(memory_space=pl.ANY)
MESH = pl.DeviceIdType.MESH


def dot(a, b):
    return lax.dot_general(a, b, (((1,), (0,)), ((), ())), preferred_element_type=F32)


def dot_t(a, b):
    return lax.dot_general(a, b, (((1,), (1,)), ((), ())), preferred_element_type=F32)


def whole(shape):
    return pl.BlockSpec(shape, lambda *_: (0,) * len(shape), pipeline_mode=pl.Buffered(1))


def params():
    return pltpu.CompilerParams(vmem_limit_bytes=VMEM_LIMIT, dimension_semantics=("arbitrary",))


def cost(matmuls, moved):
    return pl.CostEstimate(flops=int(2 * T * D * FF * matmuls), bytes_accessed=int(moved), transcendentals=0)


def root_mean_scale(wide):
    return lax.rsqrt(jnp.mean(wide * wide, -1, keepdims=True) + 1e-6)


def forward_first(x, w_gate, w_up, w_down):
    piece = 128
    pieces = D // piece

    def kernel(x_ref, wg_ref, wu_ref, wd_ref, g_ref, u_ref, t_ref, h_ref, n_ref, a_ref, held_h, acc, h_sem, n_sem):
        j = pl.program_id(0)

        @pl.when(j == 0)
        def _():
            @pl.loop(0, T // TILE)
            def _(t):
                rows = pl.ds(pl.multiple_of(t * TILE, TILE), TILE)
                wide = x_ref[rows].astype(F32)
                a_ref[rows] = (wide * root_mean_scale(wide)).astype(BF16)

        k = jnp.minimum(j, pieces - 1)
        per = D // DP // piece
        source = pl.multiple_of(block_of(k // per) * (D // DP) + lax.rem(k, per) * piece, piece)
        t_ref[...] = a_ref[:, pl.ds(source, piece)].T

        for t in range(0, T, ROWS):
            rows = slice(t, t + ROWS)
            a = a_ref[rows]
            g = dot(a, wg_ref[...])
            u = dot(a, wu_ref[...])
            g_ref[rows] = g
            u_ref[rows] = u
            act = (g * jax.nn.sigmoid(g) * u).astype(BF16)
            acc[rows] = jnp.where(j > 0, acc[rows], 0.0) + dot(act, wd_ref[...])

        @pl.when(j == CHUNKS - 1)
        def _():
            def copies(t):
                rows = pl.ds(pl.multiple_of(t * TILE, TILE), TILE)
                return (
                    pltpu.make_async_copy(held_h.at[rows], h_ref.at[rows], h_sem.at[t]),
                    pltpu.make_async_copy(a_ref.at[rows], n_ref.at[rows], n_sem.at[t]),
                )

            @pl.loop(0, T // TILE)
            def _(t):
                rows = pl.ds(pl.multiple_of(t * TILE, TILE), TILE)
                h = x_ref[rows] + acc[rows].astype(BF16)
                held_h[rows] = h
                wide = h.astype(F32)
                a_ref[rows] = (wide * root_mean_scale(wide)).astype(BF16)
                for one in copies(t):
                    one.start()

            @pl.loop(0, T // TILE)
            def _(t):
                for one in copies(t):
                    one.wait()

    tall = jax.ShapeDtypeStruct((T, FF), F32)
    flat = jax.ShapeDtypeStruct((T, D), BF16)
    wide_block = pl.BlockSpec((T, CHUNK), lambda j: (0, j))
    return pl.pallas_call(
        kernel,
        grid=(CHUNKS,),
        in_specs=[
            whole((T, D)),
            pl.BlockSpec((None, D, CHUNK), lambda j: (0, 0, j)),
            pl.BlockSpec((None, D, CHUNK), lambda j: (0, 0, j)),
            pl.BlockSpec((None, CHUNK, D), lambda j: (0, j, 0)),
        ],
        out_specs=[wide_block, wide_block, pl.BlockSpec((piece, T), lambda j: (jnp.minimum(j, pieces - 1), 0)), ANY, ANY],
        out_shape=[tall, tall, jax.ShapeDtypeStruct((D, T), BF16), flat, flat],
        scratch_shapes=[
            pltpu.VMEM((T, D), BF16),
            pltpu.VMEM((T, D), BF16),
            pltpu.VMEM((T, D), F32),
            *(pltpu.SemaphoreType.DMA((T // TILE,)),) * 2,
        ],
        compiler_params=params(),
        cost_estimate=cost(3, 90e6),
    )(x, w_gate, w_up, w_down)


def peers():
    me = lax.axis_index("dp")
    core = lax.rem(me, CORES)
    chip = me // CORES
    return chip, core, me + 1 - 2 * core, me + CORES - 2 * CORES * chip


def greet(*others):
    barrier = pltpu.get_barrier_semaphore()
    for other in others:
        pl.semaphore_signal(barrier, inc=1, device_id={"dp": other}, device_id_type=MESH)
    pl.semaphore_wait(barrier, len(others))


def block_of(i):
    chip, core, *_ = peers()
    side = lax.rem(i, CORES)
    return (side * chip + (1 - side) * (1 - chip)) * CORES + jnp.where(i < CORES, 1 - core, core)


def remote_params(ident):
    return pltpu.CompilerParams(
        vmem_limit_bytes=VMEM_LIMIT, dimension_semantics=("arbitrary",), collective_id=ident, has_side_effects=True
    )


def remote(source, landing, send_sem, recv_sem, to):
    return pltpu.make_async_remote_copy(
        src_ref=source, dst_ref=landing, send_sem=send_sem, recv_sem=recv_sem, device_id={"dp": to}, device_id_type=MESH
    )


def hidden(ident, layer, inside, lag, quick, normed, by_out, weights, gate_up, after):
    w_gate, w_up, w_down = weights
    computed = gate_up is None
    n_after = len(after)
    rows_w = D // DP
    outside = CHUNKS - inside

    def kernel(n_ref, by_ref, wd_ref, a_ref, b_ref, *rest):
        rest = rest[n_after:]
        sum_ref, far_ref, near_ref, act_ref, *rest = rest
        if computed:
            dg_ref, du_ref, n_t, *rest = rest
        else:
            n_t = n_ref
        act, out, keep, got, far, near, landed, send_sem, recv_sem, over_send, over_recv, *rest = rest
        if not computed:
            dg_ref, du_ref = rest
        j = pl.program_id(0)
        _, _, sib, opposite = peers()

        def beside(k):
            slot = lax.rem(k, 2)
            return remote(out.at[slot], got.at[k], send_sem.at[k], recv_sem.at[k], sib)

        def over(k):
            return remote(far.at[k], landed.at[k], over_send.at[k], over_recv.at[k], opposite)

        def add(k, at):
            mine = keep.at[lax.rem(k + 2, 2)]
            for which in range(2):
                far[at, which] = (mine[which, 0].astype(F32) + got[at, which, 0].astype(F32)).astype(BF16)
                near[at, which] = mine[which, 1].astype(F32) + got[at, which, 1].astype(F32)

        def finish(k, at):
            columns = pl.ds(pl.multiple_of(k * CHUNK, CHUNK), CHUNK)
            for which in range(2):
                sum_ref[which, :, columns] = (near[k, which] + landed[at, which].astype(F32)).astype(BF16)

        barrier = pltpu.get_barrier_semaphore()

        @pl.when(j == 0)
        def _():
            for other in (sib, opposite):
                pl.semaphore_signal(barrier, inc=1, device_id={"dp": other}, device_id_type=MESH)
            if computed:

                @pl.loop(0, DP)
                def _(k):
                    columns = pl.ds(pl.multiple_of(block_of(k) * rows_w, rows_w), rows_w)
                    n_t[pl.ds(pl.multiple_of(k * rows_w, rows_w), rows_w)] = n_ref[:, columns].T

        if not quick:

            @pl.when(j > 1)
            def _():
                beside(j - 2).wait()

        @pl.when((j >= lag) & (j < lag + inside))
        def _():
            over(j - lag).wait()

        for t in range(0, T, ROWS):
            rows = slice(t, t + ROWS)
            if computed:
                n = n_ref[rows]
                g, u = dot(n, a_ref[...]), dot(n, b_ref[...])
            else:
                g, u = a_ref[rows], b_ref[rows]
            p = dot_t(by_ref[rows], wd_ref[...]).astype(BF16).astype(F32)
            sig = jax.nn.sigmoid(g)
            silu = g * sig
            act[rows] = (silu * u).astype(BF16)
            du_ref[rows] = (p * silu).astype(BF16)
            dg_ref[rows] = (p * u * (sig + silu * (1.0 - sig))).astype(BF16)

        if not quick:
            add(j - 2, jnp.where(j > 1, j - 2, CHUNKS))
        finish(jnp.clip(j - lag, 0, inside - 1), jnp.where(j < lag, inside, jnp.minimum(j - lag, inside - 1)))
        act_ref[...] = act[...].T
        half = D // CORES
        for which, d_ref in ((0, dg_ref), (1, du_ref)):
            out[lax.rem(j, 2), which] = dot(n_t[:half], d_ref[...]).astype(BF16).reshape(CORES, rows_w, CHUNK)
        for which, d_ref in ((0, dg_ref), (1, du_ref)):
            keep[lax.rem(j, 2), which] = dot(n_t[half:], d_ref[...]).astype(BF16).reshape(CORES, rows_w, CHUNK)

        @pl.when(j == 0)
        def _():
            pl.semaphore_wait(barrier, 2)

        beside(j).start()
        late = 1 if quick else 2

        def meet(k):
            beside(k).wait()
            add(k, k)

        if quick:

            @pl.when(j == 0)
            def _():
                meet(0)
                over(0).start()

            @pl.when(j > 1)
            def _():
                meet(j - 1)

        @pl.when((j >= 2) & (j < inside + late))
        def _():
            over(j - late).start()

        @pl.when(j == CHUNKS - 1)
        def _():
            pl.loop(CHUNKS - late, CHUNKS)(meet)

            @pl.loop(inside, CHUNKS)
            def _(k):
                columns = pl.ds(pl.multiple_of((k - inside) * CHUNK, CHUNK), CHUNK)
                for which in range(2):
                    far_ref[which, :, columns], near_ref[which, :, columns] = far[k, which], near[k, which]

            @pl.loop(CHUNKS - lag, inside)
            def _(k):
                over(k).wait()
                finish(k, k)

    column = pl.BlockSpec((None, D, CHUNK), lambda j: (layer, 0, j))
    block = pl.BlockSpec((T, CHUNK), lambda j: (0, j))
    inner, outer = (2, rows_w, inside * CHUNK), (2, rows_w, outside * CHUNK)
    turned = pl.BlockSpec((CHUNK, T), lambda j: (j, 0))
    out_specs = [whole(inner), whole(outer), whole(outer), turned]
    out_shape = [(inner, BF16), (outer, BF16), (outer, F32), ((FF, T), BF16)]
    part, block_part = (2, CORES, rows_w, CHUNK), (2, rows_w, CHUNK)
    scratch = [
        pltpu.VMEM((T, CHUNK), BF16),
        pltpu.VMEM((2, *part), BF16),
        pltpu.VMEM((2, *part), BF16),
        pltpu.VMEM((CHUNKS + 1, *part), BF16),
        pltpu.VMEM((CHUNKS + 1, *block_part), BF16),
        pltpu.VMEM((CHUNKS + 1, *block_part), F32),
        pltpu.VMEM((inside + 1, *block_part), BF16),
        *(pltpu.SemaphoreType.DMA((CHUNKS,)),) * 2,
        *(pltpu.SemaphoreType.DMA((inside,)),) * 2,
    ]
    if computed:
        out_specs += [block, block]
        out_shape += [((T, FF), BF16)] * 2
        scratch = [pltpu.VMEM((D, T), BF16), *scratch]
    else:
        scratch += [pltpu.VMEM((T, CHUNK), BF16)] * 2
    return pl.pallas_call(
        kernel,
        grid=(CHUNKS,),
        in_specs=[
            whole(normed.shape),
            whole((T, D)),
            pl.BlockSpec((None, CHUNK, D), lambda j: (layer, j, 0)),
            *((column, column) if computed else (block, block)),
            *(ANY,) * n_after,
        ],
        out_specs=out_specs,
        out_shape=[jax.ShapeDtypeStruct(*one) for one in out_shape],
        scratch_shapes=scratch,
        compiler_params=remote_params(ident),
        cost_estimate=cost(5 if computed else 3, 60e6),
    )(normed, by_out, w_down, *((w_gate, w_up) if computed else gate_up), *after)


def down_grad(ident, act_t, by_out, parts, after):
    n_after = len(after)
    rows_w = FF // DP

    def kernel(act_ref, by_ref, *rest):
        *far_refs, near_ref, out, got, send_sem, recv_sem = rest[n_after:]
        i = pl.program_id(0)
        sib = peers()[2]

        def copy(k):
            return remote(out.at[k], got.at[k], send_sem.at[k], recv_sem.at[k], sib)

        barrier = pltpu.get_barrier_semaphore()

        @pl.when(i == 0)
        def _():
            pl.semaphore_signal(barrier, inc=1, device_id={"dp": sib}, device_id_type=MESH)

        @pl.when(i == 1)
        def _():
            pl.semaphore_wait(barrier, 1)

        term = dot(act_ref[...], by_ref[...]).astype(BF16)

        @pl.when(i < CORES)
        def _():
            out[lax.rem(i, CORES)] = term

        for k in range(CORES):

            @pl.when(i == k + 1)
            def _(k=k):
                copy(k).start()

        @pl.when(i == CORES)
        def _():
            copy(0).wait()
            far = (term.astype(F32) + got[0].astype(F32)).astype(BF16)
            for k, far_ref in enumerate(far_refs):
                far_ref[...] = far[:, k * D // parts : (k + 1) * D // parts]

        @pl.when(i == CORES + 1)
        def _():
            copy(1).wait()
            near_ref[...] = term.astype(F32) + got[1].astype(F32)

    shape, far_shape = (rows_w, D), (rows_w, D // parts)
    return pl.pallas_call(
        kernel,
        grid=(DP,),
        in_specs=[
            pl.BlockSpec((rows_w, T), lambda i: (block_of(i), 0)),
            whole((T, D)),
            *(ANY,) * n_after,
        ],
        out_specs=[*(whole(far_shape),) * parts, whole(shape)],
        out_shape=[*(jax.ShapeDtypeStruct(far_shape, BF16),) * parts, jax.ShapeDtypeStruct(shape, F32)],
        scratch_shapes=[
            pltpu.VMEM((CORES, *shape), BF16),
            pltpu.VMEM((CORES, *shape), BF16),
            pltpu.SemaphoreType.DMA((CORES,)),
            pltpu.SemaphoreType.DMA((CORES,)),
        ],
        compiler_params=remote_params(ident),
        cost_estimate=cost(1, 20e6),
    )(act_t, by_out, *after)


def clip_and_first(ident, squares, g, m, v, w):
    rows, columns = g.shape
    tile = 16

    def kernel(squares_ref, g_ref, m_ref, v_ref, w_ref, factor_ref, out_ref, held_g, held_m, held_v, held_w, mine, theirs, load, send_sem, recv_sem):
        chip, core, sib, opposite = peers()
        own = pl.ds(pl.multiple_of((chip * CORES + core) * rows, rows), rows)
        loads = [
            pltpu.make_async_copy(g_ref, held_g, load.at[0]),
            pltpu.make_async_copy(m_ref.at[0], held_m, load.at[1]),
            pltpu.make_async_copy(v_ref.at[0], held_v, load.at[2]),
            pltpu.make_async_copy(w_ref.at[0, own], held_w, load.at[3]),
        ]
        for one in loads:
            one.start()
        mine[...] = jnp.full(mine.shape, squares_ref[0], F32)
        others = (sib, opposite, opposite + 1 - 2 * core)
        greet(*others)
        copies = [remote(mine, theirs.at[k], send_sem.at[k], recv_sem.at[k], other) for k, other in enumerate(others)]
        for one in copies:
            one.start()
        for one in copies:
            one.wait()
        total = (mine[...] + theirs[0]) + (theirs[1] + theirs[2])
        factor = jnp.minimum(1.0, 0.5 * lax.rsqrt(total / COUNT + 1e-30))
        factor_ref[...] = factor
        for one in loads:
            one.wait()

        @pl.loop(0, rows // tile)
        def _(t):
            at = pl.ds(pl.multiple_of(t * tile, tile), tile)
            out_ref[at] = updated(factor[:1, :1], held_g[at], held_m[at], held_v[at], held_w[at])

    return pl.pallas_call(
        kernel,
        in_specs=[pl.BlockSpec(memory_space=pltpu.SMEM), *(ANY,) * 4],
        out_specs=[pl.BlockSpec(memory_space=pltpu.VMEM)] * 2,
        out_shape=[jax.ShapeDtypeStruct((8, 128), F32), jax.ShapeDtypeStruct((rows, columns), BF16)],
        scratch_shapes=[
            pltpu.VMEM((rows, columns), BF16),
            pltpu.VMEM((rows, columns), F32),
            pltpu.VMEM((rows, columns), F32),
            pltpu.VMEM((rows, columns), BF16),
            pltpu.VMEM((8, 128), F32),
            pltpu.VMEM((DP - 1, 8, 128), F32),
            pltpu.SemaphoreType.DMA((4,)),
            pltpu.SemaphoreType.DMA((DP - 1,)),
            pltpu.SemaphoreType.DMA((DP - 1,)),
        ],
        compiler_params=pltpu.CompilerParams(vmem_limit_bytes=VMEM_LIMIT, collective_id=ident, has_side_effects=True),
        cost_estimate=cost(0.1, 10e6),
    )(squares.reshape(1), g, m, v, w)


def updated(factor, g, m, v, w):
    g = g.astype(F32) * factor
    m = 0.9 * m + 0.1 * g
    v = 0.95 * v + 0.05 * g * g
    w = w.astype(F32)
    return (w - 0.02 * (m * lax.rsqrt(v + 1e-8) + 0.1 * w)).astype(BF16)


def new_weight(layer, me, factor, g, m, v, w, full):
    rows, columns = g.shape
    steps = 4
    tile = rows // steps
    n_full = full is not None

    def kernel(me_ref, factor_ref, g_ref, m_ref, v_ref, w_ref, *rest):
        out_ref, full_ref = rest[n_full:]
        factor = factor_ref[:1, :1]

        @pl.loop(0, tile // 16)
        def _(t):
            at = pl.ds(pl.multiple_of(t * 16, 16), 16)
            out_ref[at] = full_ref[at] = updated(factor, g_ref[at], m_ref[at], v_ref[at], w_ref[at])

    mine = pl.BlockSpec((tile, columns), lambda i, _: (i, 0))
    state = pl.BlockSpec((None, tile, columns), lambda i, _: (layer, i, 0))
    own = pl.BlockSpec((None, tile, columns), lambda i, me_ref: (layer, me_ref[0] * steps + i, 0))
    return pl.pallas_call(
        kernel,
        grid_spec=pltpu.PrefetchScalarGridSpec(
            num_scalar_prefetch=1,
            grid=(steps,),
            in_specs=[whole((8, 128)), mine, state, state, own, *(ANY,) * n_full],
            out_specs=[mine, own],
        ),
        out_shape=[jax.ShapeDtypeStruct((rows, columns), BF16), jax.ShapeDtypeStruct(w.shape, BF16)],
        input_output_aliases={6: 1} if n_full else {},
        compiler_params=params(),
        cost_estimate=cost(0.1, 10e6),
    )(me.reshape(1), factor, g, m, v, w, *((full,) if n_full else ()))


def into_states(dg, du, w_gate, w_up, h, by_out, after):
    tile = 256
    n_after = len(after)

    def kernel(dg_ref, du_ref, wg_ref, wu_ref, h_ref, by_ref, *rest):
        out_ref = rest[n_after]
        by_a = dot_t(dg_ref[...], wg_ref[...]).astype(BF16) + dot_t(du_ref[...], wu_ref[...]).astype(BF16)
        c, wide = by_a.astype(F32), h_ref[...].astype(F32)
        scale = root_mean_scale(wide)
        along = jnp.sum(c * wide, -1, keepdims=True)
        out_ref[...] = by_ref[...] + (c * scale - wide * (scale * scale * scale * along * (1.0 / D))).astype(BF16)

    long = pl.BlockSpec((tile, FF), lambda i: (i, 0))
    short = pl.BlockSpec((tile, D), lambda i: (i, 0))
    weight = pl.BlockSpec((None, D, FF), lambda i: (1, 0, 0), pipeline_mode=pl.Buffered(1))
    return pl.pallas_call(
        kernel,
        grid=(T // tile,),
        in_specs=[long, long, weight, weight, short, short, *(ANY,) * n_after],
        out_specs=short,
        out_shape=jax.ShapeDtypeStruct((T, D), BF16),
        compiler_params=params(),
        cost_estimate=cost(2, 50e6),
    )(dg, du, w_gate, w_up, h, by_out, *after)


def solution(mesh):
    sibling = [(i, i ^ 1) for i in range(DP)]
    across = [(i, i ^ 2) for i in range(DP)]

    def step(x, dy, w_gate, w_up, w_down, m_gate, m_up, m_down, v_gate, v_up, v_down):
        x, dy = x[0], dy[0]
        me = lax.axis_index("dp")
        weights = (w_gate, w_up, w_down)

        def cross(far):
            return lax.ppermute(far, "dp", across)

        g1, u1, a1, h1, a2 = forward_first(x, *weights)
        units = {}
        sum_b, far, near, act2, dg2, du2 = hidden(0, 1, 8, 6, False, a2, dy, weights, None, ())
        units["b"] = near, cross(far)
        far, near = down_grad(1, act2, dy, 1, (far,))
        units["d"] = near, cross(far)
        dh1 = into_states(dg2, du2, w_gate, w_up, h1, dy, (far,))
        sum_e, far, near, act1 = hidden(2, 0, 7, 7, True, a1, dh1, weights, (g1, u1), ())
        units["e"] = near, cross(far)
        *fars, near = down_grad(3, act1, dh1, 2, (far,))
        for k, far in enumerate(fars):
            units[f"f{k}"] = near[:, k * D // 2 : (k + 1) * D // 2], cross(far)

        nears = {name: near for name, (near, _) in units.items()}
        nears, sum_b, sum_e, _ = lax.optimization_barrier((nears, sum_b, sum_e, fars))
        units = {name: (nears[name], landed) for name, (_, landed) in units.items()}
        grads, squared = {}, []
        for name, (near, landed) in units.items():
            grads[name] = (near + landed.astype(F32)).astype(BF16)
            squared.append(jnp.sum(grads[name].astype(F32) ** 2))
            if name in "be":
                inner = sum_b if name == "b" else sum_e
                squared.append(jnp.sum(inner.astype(F32) ** 2))
                grads[name] = jnp.concatenate([inner, grads[name]], 2)

        def of(which, layer):
            if which == 2:
                return grads["d"] if layer else jnp.concatenate([grads["f0"], grads["f1"]], 1)
            return grads["b" if layer else "e"][which]

        each = {(which, layer): of(which, layer) for which in range(3) for layer in range(2)}
        late = each.pop((2, 0))
        squares, each = lax.optimization_barrier((sum(squared), each))
        each[2, 0] = late

        ms, vs = (m_gate, m_up, m_down), (v_gate, v_up, v_down)
        full, sent = [None] * 3, []
        for (which, layer), g in sorted(each.items(), key=lambda one: one[0]):
            name = f"{which}{layer}"
            if not sent:
                factor, mine = clip_and_first(4, squares, g, ms[which], vs[which], weights[which])
            else:
                mine, full[which] = new_weight(layer, me, factor, g, ms[which], vs[which], weights[which], full[which])
            over = lax.ppermute(mine, "dp", across)
            beside = lax.ppermute(mine, "dp", sibling)
            sent.append((which, layer, over, beside))
            first = mine if which + layer == 0 else first
        factor, _ = lax.optimization_barrier((factor[0, 0], mine))
        new_m, new_v = [], []
        for which in range(3):
            g = jnp.stack([each[which, 0], each[which, 1]]).astype(F32) * factor
            new_m.append(0.9 * ms[which] + 0.1 * g)
            new_v.append(0.95 * vs[which] + 0.05 * g * g)
        for k, (which, layer, over, beside) in enumerate(sent):
            if 1 <= k <= 3:
                full, new_m[k - 1], new_v[k - 1] = lax.optimization_barrier((full, new_m[k - 1], new_v[k - 1]))

            def put(piece, who):
                full[which] = lax.dynamic_update_slice(full[which], piece[None], (layer, who * piece.shape[0], 0))

            if k == 0:
                put(first, me)
            put(beside, me ^ 1)
            over, full = lax.optimization_barrier((over, full))
            corner = lax.ppermute(over, "dp", sibling)
            put(over, me ^ 2)
            put(corner, me ^ 3)
        return (*full, *new_m, *new_v)

    batch, replicated, rows = P(("rep", "dp"), None, None), P(None, None, None), P(None, "dp", None)
    return jax.shard_map(
        step,
        mesh=mesh,
        in_specs=(batch, batch, *(replicated,) * 3, *(rows,) * 6),
        out_specs=(*(P("rep", None, None),) * 3, *(P("rep", "dp", None),) * 6),
        check_vma=False,
    )
```

```python
import jax
import jax.numpy as jnp
from jax import lax
from jax.experimental import pallas as pl
from jax.experimental.pallas import tpu as pltpu
from jax.sharding import PartitionSpec as P


F32, BF16 = jnp.float32, jnp.bfloat16
T, D, FF, DP, CORES = 2048, 1024, 2816, 4, 2
COUNT = 3 * 2 * D * FF
CHUNK = 256
CHUNKS = FF // CHUNK
ROWS = 512
TILE = 256
VMEM_LIMIT = 62 * 2**20
ANY = pl.BlockSpec(memory_space=pl.ANY)
MESH = pl.DeviceIdType.MESH


def dot(a, b):
    return lax.dot_general(a, b, (((1,), (0,)), ((), ())), preferred_element_type=F32)


def dot_t(a, b):
    return lax.dot_general(a, b, (((1,), (1,)), ((), ())), preferred_element_type=F32)


def whole(shape):
    return pl.BlockSpec(shape, lambda *_: (0,) * len(shape), pipeline_mode=pl.Buffered(1))


def params():
    return pltpu.CompilerParams(vmem_limit_bytes=VMEM_LIMIT, dimension_semantics=("arbitrary",))


def cost(matmuls, moved):
    return pl.CostEstimate(flops=int(2 * T * D * FF * matmuls), bytes_accessed=int(moved), transcendentals=0)


def root_mean_scale(wide):
    return lax.rsqrt(jnp.mean(wide * wide, -1, keepdims=True) + 1e-6)


def forward_first(x, w_gate, w_up, w_down):
    piece = 128
    pieces = D // piece

    def kernel(x_ref, wg_ref, wu_ref, wd_ref, g_ref, u_ref, t_ref, h_ref, n_ref, a_ref, held_h, acc, h_sem, n_sem):
        j = pl.program_id(0)

        @pl.when(j == 0)
        def _():
            @pl.loop(0, T // TILE)
            def _(t):
                rows = pl.ds(pl.multiple_of(t * TILE, TILE), TILE)
                wide = x_ref[rows].astype(F32)
                a_ref[rows] = (wide * root_mean_scale(wide)).astype(BF16)

        k = jnp.minimum(j, pieces - 1)
        per = D // DP // piece
        source = pl.multiple_of(block_of(k // per) * (D // DP) + lax.rem(k, per) * piece, piece)
        t_ref[...] = a_ref[:, pl.ds(source, piece)].T

        for t in range(0, T, ROWS):
            rows = slice(t, t + ROWS)
            a = a_ref[rows]
            g = dot(a, wg_ref[...])
            u = dot(a, wu_ref[...])
            g_ref[rows] = g
            u_ref[rows] = u
            act = (g * jax.nn.sigmoid(g) * u).astype(BF16)
            acc[rows] = jnp.where(j > 0, acc[rows], 0.0) + dot(act, wd_ref[...])

        @pl.when(j == CHUNKS - 1)
        def _():
            def copies(t):
                rows = pl.ds(pl.multiple_of(t * TILE, TILE), TILE)
                return (
                    pltpu.make_async_copy(held_h.at[rows], h_ref.at[rows], h_sem.at[t]),
                    pltpu.make_async_copy(a_ref.at[rows], n_ref.at[rows], n_sem.at[t]),
                )

            @pl.loop(0, T // TILE)
            def _(t):
                rows = pl.ds(pl.multiple_of(t * TILE, TILE), TILE)
                h = x_ref[rows] + acc[rows].astype(BF16)
                held_h[rows] = h
                wide = h.astype(F32)
                a_ref[rows] = (wide * root_mean_scale(wide)).astype(BF16)
                for one in copies(t):
                    one.start()

            @pl.loop(0, T // TILE)
            def _(t):
                for one in copies(t):
                    one.wait()

    tall = jax.ShapeDtypeStruct((T, FF), F32)
    flat = jax.ShapeDtypeStruct((T, D), BF16)
    wide_block = pl.BlockSpec((T, CHUNK), lambda j: (0, j))
    return pl.pallas_call(
        kernel,
        grid=(CHUNKS,),
        in_specs=[
            whole((T, D)),
            pl.BlockSpec((None, D, CHUNK), lambda j: (0, 0, j)),
            pl.BlockSpec((None, D, CHUNK), lambda j: (0, 0, j)),
            pl.BlockSpec((None, CHUNK, D), lambda j: (0, j, 0)),
        ],
        out_specs=[wide_block, wide_block, pl.BlockSpec((piece, T), lambda j: (jnp.minimum(j, pieces - 1), 0)), ANY, ANY],
        out_shape=[tall, tall, jax.ShapeDtypeStruct((D, T), BF16), flat, flat],
        scratch_shapes=[
            pltpu.VMEM((T, D), BF16),
            pltpu.VMEM((T, D), BF16),
            pltpu.VMEM((T, D), F32),
            *(pltpu.SemaphoreType.DMA((T // TILE,)),) * 2,
        ],
        compiler_params=params(),
        cost_estimate=cost(3, 90e6),
    )(x, w_gate, w_up, w_down)


def peers():
    me = lax.axis_index("dp")
    core = lax.rem(me, CORES)
    chip = me // CORES
    return chip, core, me + 1 - 2 * core, me + CORES - 2 * CORES * chip


def greet(*others):
    barrier = pltpu.get_barrier_semaphore()
    for other in others:
        pl.semaphore_signal(barrier, inc=1, device_id={"dp": other}, device_id_type=MESH)
    pl.semaphore_wait(barrier, len(others))


def block_of(i):
    chip, core, *_ = peers()
    side = lax.rem(i, CORES)
    return (side * chip + (1 - side) * (1 - chip)) * CORES + jnp.where(i < CORES, 1 - core, core)


def remote_params(ident):
    return pltpu.CompilerParams(
        vmem_limit_bytes=VMEM_LIMIT, dimension_semantics=("arbitrary",), collective_id=ident, has_side_effects=True
    )


def remote(source, landing, send_sem, recv_sem, to):
    return pltpu.make_async_remote_copy(
        src_ref=source, dst_ref=landing, send_sem=send_sem, recv_sem=recv_sem, device_id={"dp": to}, device_id_type=MESH
    )


def hidden(ident, layer, inside, lag, quick, normed, by_out, weights, gate_up, after):
    w_gate, w_up, w_down = weights
    computed = gate_up is None
    n_after = len(after)
    rows_w = D // DP
    outside = CHUNKS - inside

    def kernel(n_ref, by_ref, wd_ref, a_ref, b_ref, *rest):
        rest = rest[n_after:]
        sum_ref, far_ref, near_ref, act_ref, *rest = rest
        if computed:
            dg_ref, du_ref, n_t, *rest = rest
        else:
            n_t = n_ref
        act, out, keep, got, far, near, landed, send_sem, recv_sem, over_send, over_recv, *rest = rest
        if not computed:
            dg_ref, du_ref = rest
        j = pl.program_id(0)
        _, _, sib, opposite = peers()

        def beside(k):
            slot = lax.rem(k, 2)
            return remote(out.at[slot], got.at[k], send_sem.at[k], recv_sem.at[k], sib)

        def over(k):
            return remote(far.at[k], landed.at[k], over_send.at[k], over_recv.at[k], opposite)

        def add(k, at):
            mine = keep.at[lax.rem(k + 2, 2)]
            for which in range(2):
                far[at, which] = (mine[which, 0].astype(F32) + got[at, which, 0].astype(F32)).astype(BF16)
                near[at, which] = mine[which, 1].astype(F32) + got[at, which, 1].astype(F32)

        def finish(k, at):
            columns = pl.ds(pl.multiple_of(k * CHUNK, CHUNK), CHUNK)
            for which in range(2):
                sum_ref[which, :, columns] = (near[k, which] + landed[at, which].astype(F32)).astype(BF16)

        barrier = pltpu.get_barrier_semaphore()

        @pl.when(j == 0)
        def _():
            for other in (sib, opposite):
                pl.semaphore_signal(barrier, inc=1, device_id={"dp": other}, device_id_type=MESH)
            if computed:

                @pl.loop(0, DP)
                def _(k):
                    columns = pl.ds(pl.multiple_of(block_of(k) * rows_w, rows_w), rows_w)
                    n_t[pl.ds(pl.multiple_of(k * rows_w, rows_w), rows_w)] = n_ref[:, columns].T

        if not quick:

            @pl.when(j > 1)
            def _():
                beside(j - 2).wait()

        @pl.when((j >= lag) & (j < lag + inside))
        def _():
            over(j - lag).wait()

        for t in range(0, T, ROWS):
            rows = slice(t, t + ROWS)
            if computed:
                n = n_ref[rows]
                g, u = dot(n, a_ref[...]), dot(n, b_ref[...])
            else:
                g, u = a_ref[rows], b_ref[rows]
            p = dot_t(by_ref[rows], wd_ref[...]).astype(BF16).astype(F32)
            sig = jax.nn.sigmoid(g)
            silu = g * sig
            act[rows] = (silu * u).astype(BF16)
            du_ref[rows] = (p * silu).astype(BF16)
            dg_ref[rows] = (p * u * (sig + silu * (1.0 - sig))).astype(BF16)

        if not quick:
            add(j - 2, jnp.where(j > 1, j - 2, CHUNKS))
        finish(jnp.clip(j - lag, 0, inside - 1), jnp.where(j < lag, inside, jnp.minimum(j - lag, inside - 1)))
        act_ref[...] = act[...].T
        half = D // CORES
        for which, d_ref in ((0, dg_ref), (1, du_ref)):
            out[lax.rem(j, 2), which] = dot(n_t[:half], d_ref[...]).astype(BF16).reshape(CORES, rows_w, CHUNK)
        for which, d_ref in ((0, dg_ref), (1, du_ref)):
            keep[lax.rem(j, 2), which] = dot(n_t[half:], d_ref[...]).astype(BF16).reshape(CORES, rows_w, CHUNK)

        @pl.when(j == 0)
        def _():
            pl.semaphore_wait(barrier, 2)

        beside(j).start()
        late = 1 if quick else 2

        def meet(k):
            beside(k).wait()
            add(k, k)

        if quick:

            @pl.when(j == 0)
            def _():
                meet(0)
                over(0).start()

            @pl.when(j > 1)
            def _():
                meet(j - 1)

        @pl.when((j >= 2) & (j < inside + late))
        def _():
            over(j - late).start()

        @pl.when(j == CHUNKS - 1)
        def _():
            pl.loop(CHUNKS - late, CHUNKS)(meet)

            @pl.loop(inside, CHUNKS)
            def _(k):
                columns = pl.ds(pl.multiple_of((k - inside) * CHUNK, CHUNK), CHUNK)
                for which in range(2):
                    far_ref[which, :, columns], near_ref[which, :, columns] = far[k, which], near[k, which]

            @pl.loop(CHUNKS - lag, inside)
            def _(k):
                over(k).wait()
                finish(k, k)

    column = pl.BlockSpec((None, D, CHUNK), lambda j: (layer, 0, j))
    block = pl.BlockSpec((T, CHUNK), lambda j: (0, j))
    inner, outer = (2, rows_w, inside * CHUNK), (2, rows_w, outside * CHUNK)
    turned = pl.BlockSpec((CHUNK, T), lambda j: (j, 0))
    out_specs = [whole(inner), whole(outer), whole(outer), turned]
    out_shape = [(inner, BF16), (outer, BF16), (outer, F32), ((FF, T), BF16)]
    part, block_part = (2, CORES, rows_w, CHUNK), (2, rows_w, CHUNK)
    scratch = [
        pltpu.VMEM((T, CHUNK), BF16),
        pltpu.VMEM((2, *part), BF16),
        pltpu.VMEM((2, *part), BF16),
        pltpu.VMEM((CHUNKS + 1, *part), BF16),
        pltpu.VMEM((CHUNKS + 1, *block_part), BF16),
        pltpu.VMEM((CHUNKS + 1, *block_part), F32),
        pltpu.VMEM((inside + 1, *block_part), BF16),
        *(pltpu.SemaphoreType.DMA((CHUNKS,)),) * 2,
        *(pltpu.SemaphoreType.DMA((inside,)),) * 2,
    ]
    if computed:
        out_specs += [block, block]
        out_shape += [((T, FF), BF16)] * 2
        scratch = [pltpu.VMEM((D, T), BF16), *scratch]
    else:
        scratch += [pltpu.VMEM((T, CHUNK), BF16)] * 2
    return pl.pallas_call(
        kernel,
        grid=(CHUNKS,),
        in_specs=[
            whole(normed.shape),
            whole((T, D)),
            pl.BlockSpec((None, CHUNK, D), lambda j: (layer, j, 0)),
            *((column, column) if computed else (block, block)),
            *(ANY,) * n_after,
        ],
        out_specs=out_specs,
        out_shape=[jax.ShapeDtypeStruct(*one) for one in out_shape],
        scratch_shapes=scratch,
        compiler_params=remote_params(ident),
        cost_estimate=cost(5 if computed else 3, 60e6),
    )(normed, by_out, w_down, *((w_gate, w_up) if computed else gate_up), *after)


def down_grad(ident, act_t, by_out, parts, after):
    n_after = len(after)
    rows_w = FF // DP

    def kernel(act_ref, by_ref, *rest):
        *far_refs, near_ref, out, got, send_sem, recv_sem = rest[n_after:]
        i = pl.program_id(0)
        sib = peers()[2]

        def copy(k):
            return remote(out.at[k], got.at[k], send_sem.at[k], recv_sem.at[k], sib)

        barrier = pltpu.get_barrier_semaphore()

        @pl.when(i == 0)
        def _():
            pl.semaphore_signal(barrier, inc=1, device_id={"dp": sib}, device_id_type=MESH)

        @pl.when(i == 1)
        def _():
            pl.semaphore_wait(barrier, 1)

        term = dot(act_ref[...], by_ref[...]).astype(BF16)

        @pl.when(i < CORES)
        def _():
            out[lax.rem(i, CORES)] = term

        for k in range(CORES):

            @pl.when(i == k + 1)
            def _(k=k):
                copy(k).start()

        @pl.when(i == CORES)
        def _():
            copy(0).wait()
            far = (term.astype(F32) + got[0].astype(F32)).astype(BF16)
            for (start, stop), far_ref in zip(parts, far_refs, strict=True):
                far_ref[...] = far[:, start:stop]

        @pl.when(i == CORES + 1)
        def _():
            copy(1).wait()
            near_ref[...] = term.astype(F32) + got[1].astype(F32)

    shape = (rows_w, D)
    far_shapes = [(rows_w, stop - start) for start, stop in parts]
    return pl.pallas_call(
        kernel,
        grid=(DP,),
        in_specs=[
            pl.BlockSpec((rows_w, T), lambda i: (block_of(i), 0)),
            whole((T, D)),
            *(ANY,) * n_after,
        ],
        out_specs=[*map(whole, far_shapes), whole(shape)],
        out_shape=[*(jax.ShapeDtypeStruct(one, BF16) for one in far_shapes), jax.ShapeDtypeStruct(shape, F32)],
        scratch_shapes=[
            pltpu.VMEM((CORES, *shape), BF16),
            pltpu.VMEM((CORES, *shape), BF16),
            pltpu.SemaphoreType.DMA((CORES,)),
            pltpu.SemaphoreType.DMA((CORES,)),
        ],
        compiler_params=remote_params(ident),
        cost_estimate=cost(1, 20e6),
    )(act_t, by_out, *after)


def clip_and_first(ident, squares, g, m, v, w):
    rows, columns = g.shape
    tile = 16

    def kernel(squares_ref, g_ref, m_ref, v_ref, w_ref, factor_ref, out_ref, held_g, held_m, held_v, held_w, mine, theirs, load, send_sem, recv_sem):
        chip, core, sib, opposite = peers()
        own = pl.ds(pl.multiple_of((chip * CORES + core) * rows, rows), rows)
        loads = [
            pltpu.make_async_copy(g_ref, held_g, load.at[0]),
            pltpu.make_async_copy(m_ref.at[0], held_m, load.at[1]),
            pltpu.make_async_copy(v_ref.at[0], held_v, load.at[2]),
            pltpu.make_async_copy(w_ref.at[0, own], held_w, load.at[3]),
        ]
        for one in loads:
            one.start()
        mine[...] = jnp.full(mine.shape, squares_ref[0], F32)
        others = (sib, opposite, opposite + 1 - 2 * core)
        greet(*others)
        copies = [remote(mine, theirs.at[k], send_sem.at[k], recv_sem.at[k], other) for k, other in enumerate(others)]
        for one in copies:
            one.start()
        for one in copies:
            one.wait()
        total = (mine[...] + theirs[0]) + (theirs[1] + theirs[2])
        factor = jnp.minimum(1.0, 0.5 * lax.rsqrt(total / COUNT + 1e-30))
        factor_ref[...] = factor
        for one in loads:
            one.wait()

        @pl.loop(0, rows // tile)
        def _(t):
            at = pl.ds(pl.multiple_of(t * tile, tile), tile)
            out_ref[at] = updated(factor[:1, :1], held_g[at], held_m[at], held_v[at], held_w[at])

    return pl.pallas_call(
        kernel,
        in_specs=[pl.BlockSpec(memory_space=pltpu.SMEM), *(ANY,) * 4],
        out_specs=[pl.BlockSpec(memory_space=pltpu.VMEM)] * 2,
        out_shape=[jax.ShapeDtypeStruct((8, 128), F32), jax.ShapeDtypeStruct((rows, columns), BF16)],
        scratch_shapes=[
            pltpu.VMEM((rows, columns), BF16),
            pltpu.VMEM((rows, columns), F32),
            pltpu.VMEM((rows, columns), F32),
            pltpu.VMEM((rows, columns), BF16),
            pltpu.VMEM((8, 128), F32),
            pltpu.VMEM((DP - 1, 8, 128), F32),
            pltpu.SemaphoreType.DMA((4,)),
            pltpu.SemaphoreType.DMA((DP - 1,)),
            pltpu.SemaphoreType.DMA((DP - 1,)),
        ],
        compiler_params=pltpu.CompilerParams(vmem_limit_bytes=VMEM_LIMIT, collective_id=ident, has_side_effects=True),
        cost_estimate=cost(0.1, 10e6),
    )(squares.reshape(1), g, m, v, w)


def updated(factor, g, m, v, w):
    g = g.astype(F32) * factor
    m = 0.9 * m + 0.1 * g
    v = 0.95 * v + 0.05 * g * g
    w = w.astype(F32)
    return (w - 0.02 * (m * lax.rsqrt(v + 1e-8) + 0.1 * w)).astype(BF16)


def new_weight(layer, me, factor, g, m, v, w, full):
    rows, columns = g.shape
    steps = 4
    tile = rows // steps
    n_full = full is not None

    def kernel(me_ref, factor_ref, g_ref, m_ref, v_ref, w_ref, *rest):
        out_ref, full_ref = rest[n_full:]
        factor = factor_ref[:1, :1]

        @pl.loop(0, tile // 16)
        def _(t):
            at = pl.ds(pl.multiple_of(t * 16, 16), 16)
            out_ref[at] = full_ref[at] = updated(factor, g_ref[at], m_ref[at], v_ref[at], w_ref[at])

    mine = pl.BlockSpec((tile, columns), lambda i, _: (i, 0))
    state = pl.BlockSpec((None, tile, columns), lambda i, _: (layer, i, 0))
    own = pl.BlockSpec((None, tile, columns), lambda i, me_ref: (layer, me_ref[0] * steps + i, 0))
    return pl.pallas_call(
        kernel,
        grid_spec=pltpu.PrefetchScalarGridSpec(
            num_scalar_prefetch=1,
            grid=(steps,),
            in_specs=[whole((8, 128)), mine, state, state, own, *(ANY,) * n_full],
            out_specs=[mine, own],
        ),
        out_shape=[jax.ShapeDtypeStruct((rows, columns), BF16), jax.ShapeDtypeStruct(w.shape, BF16)],
        input_output_aliases={6: 1} if n_full else {},
        compiler_params=params(),
        cost_estimate=cost(0.1, 10e6),
    )(me.reshape(1), factor, g, m, v, w, *((full,) if n_full else ()))


def middle(ident, act_t, dg, du, w_gate, w_up, h, by_out, after):
    tile, rows_w, rest_columns = 256, FF // DP, D // 4
    inner = D - rest_columns
    steps = T // tile
    n_after = len(after)

    def kernel(act_ref, by_ref, dg_ref, du_ref, wg_hbm, wu_hbm, h_ref, *rest):
        rest = rest[n_after:]
        out_ref, sum_ref, far_ref, near_ref, wg, wu, out, got, far, near, landed, load, send_sem, recv_sem, over_send, over_recv = rest
        i = pl.program_id(0)
        _, _, sib, opposite = peers()
        barrier = pltpu.get_barrier_semaphore()
        loads = [
            pltpu.make_async_copy(wg_hbm.at[1], wg, load.at[0]),
            pltpu.make_async_copy(wu_hbm.at[1], wu, load.at[1]),
        ]

        def beside(k):
            return remote(out.at[k], got.at[k], send_sem.at[k], recv_sem.at[k], sib)

        def over():
            return remote(far, landed, over_send.at[0], over_recv.at[0], opposite)

        @pl.when(i == 0)
        def _():
            for one in loads:
                one.start()
            for other in (sib, opposite):
                pl.semaphore_signal(barrier, inc=1, device_id={"dp": other}, device_id_type=MESH)

        @pl.when(i == 1)
        def _():
            pl.semaphore_wait(barrier, 2)
            beside(0).start()

        @pl.when(i == 2)
        def _():
            over().start()

        @pl.when(i == 3)
        def _():
            beside(1).start()

        @pl.when(i == DP)
        def _():
            for one in loads:
                one.wait()

        @pl.when(i < DP)
        def _():
            term = dot(act_ref[...], by_ref[...]).astype(BF16)

            @pl.when(i == 0)
            def _():
                out[0] = term

            @pl.when(i == 1)
            def _():
                beside(0).wait()
                there = (term.astype(F32) + got[0].astype(F32)).astype(BF16)
                far[...] = there[:, :inner]
                far_ref[...] = there[:, inner:]

            @pl.when(i == 2)
            def _():
                out[1] = term

            @pl.when(i == 3)
            def _():
                beside(1).wait()
                here = term.astype(F32) + got[1].astype(F32)
                near[...] = here[:, :inner]
                near_ref[...] = here[:, inner:]

        @pl.when(i >= DP)
        def _():
            by_a = dot_t(dg_ref[...], wg[...]).astype(BF16) + dot_t(du_ref[...], wu[...]).astype(BF16)
            c, wide = by_a.astype(F32), h_ref[...].astype(F32)
            scale = root_mean_scale(wide)
            along = jnp.sum(c * wide, -1, keepdims=True)
            by = by_ref[pl.ds(pl.multiple_of((i - DP) * tile, tile), tile)]
            out_ref[...] = by + (c * scale - wide * (scale * scale * scale * along * (1.0 / D))).astype(BF16)

        @pl.when(i == DP + steps - 1)
        def _():
            over().wait()
            sum_ref[...] = (near[...] + landed[...].astype(F32)).astype(BF16)

    def row(i):
        return jnp.maximum(i - DP, 0)

    def source(i):
        k = jnp.minimum(i, DP - 1)
        return block_of(lax.rem(k, CORES) * CORES + k // CORES)

    long = pl.BlockSpec((tile, FF), lambda i: (row(i), 0))
    short = pl.BlockSpec((tile, D), lambda i: (row(i), 0))
    most, few = (rows_w, inner), (rows_w, rest_columns)
    return pl.pallas_call(
        kernel,
        grid=(DP + steps,),
        in_specs=[pl.BlockSpec((rows_w, T), lambda i: (source(i), 0)), whole((T, D)), long, long, ANY, ANY, short, *(ANY,) * n_after],
        out_specs=[short, whole(most), whole(few), whole(few)],
        out_shape=[
            jax.ShapeDtypeStruct((T, D), BF16),
            jax.ShapeDtypeStruct(most, BF16),
            jax.ShapeDtypeStruct(few, BF16),
            jax.ShapeDtypeStruct(few, F32),
        ],
        scratch_shapes=[
            pltpu.VMEM((D, FF), BF16),
            pltpu.VMEM((D, FF), BF16),
            pltpu.VMEM((CORES, rows_w, D), BF16),
            pltpu.VMEM((CORES, rows_w, D), BF16),
            pltpu.VMEM(most, BF16),
            pltpu.VMEM(most, F32),
            pltpu.VMEM(most, BF16),
            *(pltpu.SemaphoreType.DMA((CORES,)),) * 3,
            *(pltpu.SemaphoreType.DMA((1,)),) * 2,
        ],
        compiler_params=remote_params(ident),
        cost_estimate=cost(3, 70e6),
    )(act_t, by_out, dg, du, w_gate, w_up, h, *after)


def solution(mesh):
    sibling = [(i, i ^ 1) for i in range(DP)]
    across = [(i, i ^ 2) for i in range(DP)]

    def step(x, dy, w_gate, w_up, w_down, m_gate, m_up, m_down, v_gate, v_up, v_down):
        x, dy = x[0], dy[0]
        me = lax.axis_index("dp")
        weights = (w_gate, w_up, w_down)

        def cross(far):
            return lax.ppermute(far, "dp", across)

        g1, u1, a1, h1, a2 = forward_first(x, *weights)
        units = {}
        sum_b, far, near, act2, dg2, du2 = hidden(0, 1, 8, 6, False, a2, dy, weights, None, ())
        units["b"] = near, cross(far)
        dh1, sum_d, far, near = middle(1, act2, dg2, du2, w_gate, w_up, h1, dy, (far,))
        units["d"] = near, cross(far)
        sum_e, far, near, act1 = hidden(2, 0, 7, 7, True, a1, dh1, weights, (g1, u1), ())
        units["e"] = near, cross(far)
        parts = ((0, 3 * D // 4), (3 * D // 4, D))
        *fars, near = down_grad(3, act1, dh1, parts, (far,))
        for k, (far, (start, stop)) in enumerate(zip(fars, parts, strict=True)):
            units[f"f{k}"] = near[:, start:stop], cross(far)

        nears = {name: near for name, (near, _) in units.items()}
        nears, inners, _ = lax.optimization_barrier((nears, {"b": sum_b, "d": sum_d, "e": sum_e}, fars))
        units = {name: (nears[name], landed) for name, (_, landed) in units.items()}
        grads, squared = {}, []
        for name, (near, landed) in units.items():
            grads[name] = (near + landed.astype(F32)).astype(BF16)
            squared.append(jnp.sum(grads[name].astype(F32) ** 2))
            if name in inners:
                squared.append(jnp.sum(inners[name].astype(F32) ** 2))
                grads[name] = jnp.concatenate([inners[name], grads[name]], -1)

        def of(which, layer):
            if which == 2:
                return grads["d"] if layer else jnp.concatenate([grads["f0"], grads["f1"]], 1)
            return grads["b" if layer else "e"][which]

        each = {(which, layer): of(which, layer) for which in range(3) for layer in range(2)}
        late = each.pop((2, 0))
        squares, each = lax.optimization_barrier((sum(squared), each))
        each[2, 0] = late

        ms, vs = (m_gate, m_up, m_down), (v_gate, v_up, v_down)
        full, sent = [None] * 3, []
        for (which, layer), g in sorted(each.items(), key=lambda one: one[0]):
            name = f"{which}{layer}"
            if not sent:
                factor, mine = clip_and_first(4, squares, g, ms[which], vs[which], weights[which])
            else:
                mine, full[which] = new_weight(layer, me, factor, g, ms[which], vs[which], weights[which], full[which])
            first = mine if which + layer == 0 else first
            over = lax.ppermute(mine, "dp", across)
            beside = lax.ppermute(mine, "dp", sibling)
            sent.append((which, layer, over, beside))
        factor, _ = lax.optimization_barrier((factor[0, 0], mine))
        new_m, new_v = [], []
        for which in range(3):
            g = jnp.stack([each[which, 0], each[which, 1]]).astype(F32) * factor
            new_m.append(0.9 * ms[which] + 0.1 * g)
            new_v.append(0.95 * vs[which] + 0.05 * g * g)
        for k, (which, layer, over, beside) in enumerate(sent):
            if 1 <= k <= 3:
                full, new_m[k - 1], new_v[k - 1] = lax.optimization_barrier((full, new_m[k - 1], new_v[k - 1]))

            def put(piece, who):
                full[which] = lax.dynamic_update_slice(full[which], piece[None], (layer, who * piece.shape[0], 0))

            if k == 0:
                put(first, me)
            put(beside, me ^ 1)
            over, full = lax.optimization_barrier((over, full))
            corner = lax.ppermute(over, "dp", sibling)
            put(over, me ^ 2)
            put(corner, me ^ 3)
        return (*full, *new_m, *new_v)

    batch, replicated, rows = P(("rep", "dp"), None, None), P(None, None, None), P(None, "dp", None)
    return jax.shard_map(
        step,
        mesh=mesh,
        in_specs=(batch, batch, *(replicated,) * 3, *(rows,) * 6),
        out_specs=(*(P("rep", None, None),) * 3, *(P("rep", "dp", None),) * 6),
        check_vma=False,
    )
```

```python
import jax
import jax.numpy as jnp
from jax import lax
from jax.experimental import pallas as pl
from jax.experimental.pallas import tpu as pltpu
from jax.sharding import PartitionSpec as P


F32, BF16 = jnp.float32, jnp.bfloat16
T, D, FF, DP, CORES = 2048, 1024, 2816, 4, 2
COUNT = 3 * 2 * D * FF
CHUNK = 256
CHUNKS = FF // CHUNK
ROWS = 512
TILE = 256
VMEM_LIMIT = 62 * 2**20
ANY = pl.BlockSpec(memory_space=pl.ANY)
MESH = pl.DeviceIdType.MESH


def dot(a, b):
    return lax.dot_general(a, b, (((1,), (0,)), ((), ())), preferred_element_type=F32)


def dot_t(a, b):
    return lax.dot_general(a, b, (((1,), (1,)), ((), ())), preferred_element_type=F32)


def whole(shape):
    return pl.BlockSpec(shape, lambda *_: (0,) * len(shape), pipeline_mode=pl.Buffered(1))


def params():
    return pltpu.CompilerParams(vmem_limit_bytes=VMEM_LIMIT, dimension_semantics=("arbitrary",))


def cost(matmuls, moved):
    return pl.CostEstimate(flops=int(2 * T * D * FF * matmuls), bytes_accessed=int(moved), transcendentals=0)


def root_mean_scale(wide):
    return lax.rsqrt(jnp.mean(wide * wide, -1, keepdims=True) + 1e-6)


def forward_first(x, w_gate, w_up, w_down):
    piece = 128
    pieces = D // piece

    def kernel(x_ref, wg_ref, wu_ref, wd_ref, g_ref, u_ref, t_ref, h_ref, n_ref, a_ref, held_h, acc, h_sem, n_sem):
        j = pl.program_id(0)

        @pl.when(j == 0)
        def _():
            @pl.loop(0, T // TILE)
            def _(t):
                rows = pl.ds(pl.multiple_of(t * TILE, TILE), TILE)
                wide = x_ref[rows].astype(F32)
                a_ref[rows] = (wide * root_mean_scale(wide)).astype(BF16)

        k = jnp.minimum(j, pieces - 1)
        per = D // DP // piece
        source = pl.multiple_of(block_of(k // per) * (D // DP) + lax.rem(k, per) * piece, piece)
        t_ref[...] = a_ref[:, pl.ds(source, piece)].T

        for t in range(0, T, ROWS):
            rows = slice(t, t + ROWS)
            a = a_ref[rows]
            g = dot(a, wg_ref[...])
            u = dot(a, wu_ref[...])
            g_ref[rows] = g
            u_ref[rows] = u
            act = (g * jax.nn.sigmoid(g) * u).astype(BF16)
            acc[rows] = jnp.where(j > 0, acc[rows], 0.0) + dot(act, wd_ref[...])

        @pl.when(j == CHUNKS - 1)
        def _():
            def copies(t):
                rows = pl.ds(pl.multiple_of(t * TILE, TILE), TILE)
                return (
                    pltpu.make_async_copy(held_h.at[rows], h_ref.at[rows], h_sem.at[t]),
                    pltpu.make_async_copy(a_ref.at[rows], n_ref.at[rows], n_sem.at[t]),
                )

            @pl.loop(0, T // TILE)
            def _(t):
                rows = pl.ds(pl.multiple_of(t * TILE, TILE), TILE)
                h = x_ref[rows] + acc[rows].astype(BF16)
                held_h[rows] = h
                wide = h.astype(F32)
                a_ref[rows] = (wide * root_mean_scale(wide)).astype(BF16)
                for one in copies(t):
                    one.start()

            @pl.loop(0, T // TILE)
            def _(t):
                for one in copies(t):
                    one.wait()

    tall = jax.ShapeDtypeStruct((T, FF), F32)
    flat = jax.ShapeDtypeStruct((T, D), BF16)
    wide_block = pl.BlockSpec((T, CHUNK), lambda j: (0, j))
    return pl.pallas_call(
        kernel,
        grid=(CHUNKS,),
        in_specs=[
            whole((T, D)),
            pl.BlockSpec((None, D, CHUNK), lambda j: (0, 0, j)),
            pl.BlockSpec((None, D, CHUNK), lambda j: (0, 0, j)),
            pl.BlockSpec((None, CHUNK, D), lambda j: (0, j, 0)),
        ],
        out_specs=[wide_block, wide_block, pl.BlockSpec((piece, T), lambda j: (jnp.minimum(j, pieces - 1), 0)), ANY, ANY],
        out_shape=[tall, tall, jax.ShapeDtypeStruct((D, T), BF16), flat, flat],
        scratch_shapes=[
            pltpu.VMEM((T, D), BF16),
            pltpu.VMEM((T, D), BF16),
            pltpu.VMEM((T, D), F32),
            *(pltpu.SemaphoreType.DMA((T // TILE,)),) * 2,
        ],
        compiler_params=params(),
        cost_estimate=cost(3, 90e6),
    )(x, w_gate, w_up, w_down)


def peers():
    me = lax.axis_index("dp")
    core = lax.rem(me, CORES)
    chip = me // CORES
    return chip, core, me + 1 - 2 * core, me + CORES - 2 * CORES * chip


def greet(*others):
    barrier = pltpu.get_barrier_semaphore()
    for other in others:
        pl.semaphore_signal(barrier, inc=1, device_id={"dp": other}, device_id_type=MESH)
    pl.semaphore_wait(barrier, len(others))


def block_of(i):
    chip, core, *_ = peers()
    side = lax.rem(i, CORES)
    return (side * chip + (1 - side) * (1 - chip)) * CORES + jnp.where(i < CORES, 1 - core, core)


def remote_params(ident):
    return pltpu.CompilerParams(
        vmem_limit_bytes=VMEM_LIMIT, dimension_semantics=("arbitrary",), collective_id=ident, has_side_effects=True
    )


def remote(source, landing, send_sem, recv_sem, to):
    return pltpu.make_async_remote_copy(
        src_ref=source, dst_ref=landing, send_sem=send_sem, recv_sem=recv_sem, device_id={"dp": to}, device_id_type=MESH
    )


def hidden(ident, layer, inside, lag, quick, normed, by_out, weights, gate_up, after):
    w_gate, w_up, w_down = weights
    computed = gate_up is None
    n_after = len(after)
    rows_w = D // DP
    outside = CHUNKS - inside

    def kernel(n_ref, by_ref, wd_ref, a_ref, b_ref, *rest):
        rest = rest[n_after:]
        sum_ref, far_ref, near_ref, act_ref, *rest = rest
        if computed:
            dg_ref, du_ref, n_t, *rest = rest
        else:
            n_t = n_ref
        act, out, keep, got, far, near, landed, send_sem, recv_sem, over_send, over_recv, *rest = rest
        if not computed:
            dg_ref, du_ref = rest
        j = pl.program_id(0)
        _, _, sib, opposite = peers()

        def beside(k):
            slot = lax.rem(k, 2)
            return remote(out.at[slot], got.at[k], send_sem.at[k], recv_sem.at[k], sib)

        def over(k):
            return remote(far.at[k], landed.at[k], over_send.at[k], over_recv.at[k], opposite)

        def add(k, at):
            mine = keep.at[lax.rem(k + 2, 2)]
            for which in range(2):
                far[at, which] = (mine[which, 0].astype(F32) + got[at, which, 0].astype(F32)).astype(BF16)
                near[at, which] = mine[which, 1].astype(F32) + got[at, which, 1].astype(F32)

        def finish(k, at):
            columns = pl.ds(pl.multiple_of(k * CHUNK, CHUNK), CHUNK)
            for which in range(2):
                sum_ref[which, :, columns] = (near[k, which] + landed[at, which].astype(F32)).astype(BF16)

        barrier = pltpu.get_barrier_semaphore()

        @pl.when(j == 0)
        def _():
            for other in (sib, opposite):
                pl.semaphore_signal(barrier, inc=1, device_id={"dp": other}, device_id_type=MESH)
            if computed:

                @pl.loop(0, DP)
                def _(k):
                    columns = pl.ds(pl.multiple_of(block_of(k) * rows_w, rows_w), rows_w)
                    n_t[pl.ds(pl.multiple_of(k * rows_w, rows_w), rows_w)] = n_ref[:, columns].T

        if not quick:

            @pl.when(j > 1)
            def _():
                beside(j - 2).wait()

        @pl.when((j >= lag) & (j < lag + inside))
        def _():
            over(j - lag).wait()

        for t in range(0, T, ROWS):
            rows = slice(t, t + ROWS)
            if computed:
                n = n_ref[rows]
                g, u = dot(n, a_ref[...]), dot(n, b_ref[...])
            else:
                g, u = a_ref[rows], b_ref[rows]
            p = dot_t(by_ref[rows], wd_ref[...]).astype(BF16).astype(F32)
            sig = jax.nn.sigmoid(g)
            silu = g * sig
            act[rows] = (silu * u).astype(BF16)
            du_ref[rows] = (p * silu).astype(BF16)
            dg_ref[rows] = (p * u * (sig + silu * (1.0 - sig))).astype(BF16)

        if not quick:
            add(j - 2, jnp.where(j > 1, j - 2, CHUNKS))
        finish(jnp.clip(j - lag, 0, inside - 1), jnp.where(j < lag, inside, jnp.minimum(j - lag, inside - 1)))
        act_ref[...] = act[...].T
        half = D // CORES
        for which, d_ref in ((0, dg_ref), (1, du_ref)):
            out[lax.rem(j, 2), which] = dot(n_t[:half], d_ref[...]).astype(BF16).reshape(CORES, rows_w, CHUNK)
        for which, d_ref in ((0, dg_ref), (1, du_ref)):
            keep[lax.rem(j, 2), which] = dot(n_t[half:], d_ref[...]).astype(BF16).reshape(CORES, rows_w, CHUNK)

        @pl.when(j == 0)
        def _():
            pl.semaphore_wait(barrier, 2)

        beside(j).start()
        late = 1 if quick else 2

        def meet(k):
            beside(k).wait()
            add(k, k)

        if quick:

            @pl.when(j > 0)
            def _():
                meet(j - 1)

        @pl.when((j >= late) & (j < inside + late))
        def _():
            over(j - late).start()

        @pl.when(j == CHUNKS - 1)
        def _():
            pl.loop(CHUNKS - late, CHUNKS)(meet)

            @pl.loop(inside, CHUNKS)
            def _(k):
                columns = pl.ds(pl.multiple_of((k - inside) * CHUNK, CHUNK), CHUNK)
                for which in range(2):
                    far_ref[which, :, columns], near_ref[which, :, columns] = far[k, which], near[k, which]

            @pl.loop(CHUNKS - lag, inside)
            def _(k):
                over(k).wait()
                finish(k, k)

    column = pl.BlockSpec((None, D, CHUNK), lambda j: (layer, 0, j))
    block = pl.BlockSpec((T, CHUNK), lambda j: (0, j))
    inner, outer = (2, rows_w, inside * CHUNK), (2, rows_w, outside * CHUNK)
    turned = pl.BlockSpec((CHUNK, T), lambda j: (j, 0))
    out_specs = [whole(inner), whole(outer), whole(outer), turned]
    out_shape = [(inner, BF16), (outer, BF16), (outer, F32), ((FF, T), BF16)]
    part, block_part = (2, CORES, rows_w, CHUNK), (2, rows_w, CHUNK)
    scratch = [
        pltpu.VMEM((T, CHUNK), BF16),
        pltpu.VMEM((2, *part), BF16),
        pltpu.VMEM((2, *part), BF16),
        pltpu.VMEM((CHUNKS + 1, *part), BF16),
        pltpu.VMEM((CHUNKS + 1, *block_part), BF16),
        pltpu.VMEM((CHUNKS + 1, *block_part), F32),
        pltpu.VMEM((inside + 1, *block_part), BF16),
        *(pltpu.SemaphoreType.DMA((CHUNKS,)),) * 2,
        *(pltpu.SemaphoreType.DMA((inside,)),) * 2,
    ]
    if computed:
        out_specs += [block, block]
        out_shape += [((T, FF), BF16)] * 2
        scratch = [pltpu.VMEM((D, T), BF16), *scratch]
    else:
        scratch += [pltpu.VMEM((T, CHUNK), BF16)] * 2
    return pl.pallas_call(
        kernel,
        grid=(CHUNKS,),
        in_specs=[
            whole(normed.shape),
            whole((T, D)),
            pl.BlockSpec((None, CHUNK, D), lambda j: (layer, j, 0)),
            *((column, column) if computed else (block, block)),
            *(ANY,) * n_after,
        ],
        out_specs=out_specs,
        out_shape=[jax.ShapeDtypeStruct(*one) for one in out_shape],
        scratch_shapes=scratch,
        compiler_params=remote_params(ident),
        cost_estimate=cost(5 if computed else 3, 60e6),
    )(normed, by_out, w_down, *((w_gate, w_up) if computed else gate_up), *after)


def down_grad(ident, act_t, by_out, parts, after):
    n_after = len(after)
    rows_w = FF // DP

    def kernel(act_ref, by_ref, *rest):
        *far_refs, near_ref, out, got, send_sem, recv_sem = rest[n_after:]
        i = pl.program_id(0)
        sib = peers()[2]

        def copy(k):
            return remote(out.at[k], got.at[k], send_sem.at[k], recv_sem.at[k], sib)

        barrier = pltpu.get_barrier_semaphore()

        @pl.when(i == 0)
        def _():
            pl.semaphore_signal(barrier, inc=1, device_id={"dp": sib}, device_id_type=MESH)

        @pl.when(i == 1)
        def _():
            pl.semaphore_wait(barrier, 1)

        term = dot(act_ref[...], by_ref[...]).astype(BF16)

        @pl.when(i < CORES)
        def _():
            out[lax.rem(i, CORES)] = term

        for k in range(CORES):

            @pl.when(i == k + 1)
            def _(k=k):
                copy(k).start()

        @pl.when(i == CORES)
        def _():
            copy(0).wait()
            far = (term.astype(F32) + got[0].astype(F32)).astype(BF16)
            for (start, stop), far_ref in zip(parts, far_refs, strict=True):
                far_ref[...] = far[:, start:stop]

        @pl.when(i == CORES + 1)
        def _():
            copy(1).wait()
            near_ref[...] = term.astype(F32) + got[1].astype(F32)

    shape = (rows_w, D)
    far_shapes = [(rows_w, stop - start) for start, stop in parts]
    return pl.pallas_call(
        kernel,
        grid=(DP,),
        in_specs=[
            pl.BlockSpec((rows_w, T), lambda i: (block_of(i), 0)),
            whole((T, D)),
            *(ANY,) * n_after,
        ],
        out_specs=[*map(whole, far_shapes), whole(shape)],
        out_shape=[*(jax.ShapeDtypeStruct(one, BF16) for one in far_shapes), jax.ShapeDtypeStruct(shape, F32)],
        scratch_shapes=[
            pltpu.VMEM((CORES, *shape), BF16),
            pltpu.VMEM((CORES, *shape), BF16),
            pltpu.SemaphoreType.DMA((CORES,)),
            pltpu.SemaphoreType.DMA((CORES,)),
        ],
        compiler_params=remote_params(ident),
        cost_estimate=cost(1, 20e6),
    )(act_t, by_out, *after)


def clip_and_first(ident, squares, g, m, v, w):
    rows, columns = g.shape
    tile = 16

    def kernel(squares_ref, g_ref, m_ref, v_ref, w_ref, factor_ref, out_ref, held_g, held_m, held_v, held_w, mine, theirs, load, send_sem, recv_sem):
        chip, core, sib, opposite = peers()
        own = pl.ds(pl.multiple_of((chip * CORES + core) * rows, rows), rows)
        loads = [
            pltpu.make_async_copy(g_ref, held_g, load.at[0]),
            pltpu.make_async_copy(m_ref.at[0], held_m, load.at[1]),
            pltpu.make_async_copy(v_ref.at[0], held_v, load.at[2]),
            pltpu.make_async_copy(w_ref.at[0, own], held_w, load.at[3]),
        ]
        for one in loads:
            one.start()
        mine[...] = jnp.full(mine.shape, squares_ref[0], F32)
        others = (sib, opposite, opposite + 1 - 2 * core)
        greet(*others)
        copies = [remote(mine, theirs.at[k], send_sem.at[k], recv_sem.at[k], other) for k, other in enumerate(others)]
        for one in copies:
            one.start()
        for one in copies:
            one.wait()
        total = (mine[...] + theirs[0]) + (theirs[1] + theirs[2])
        factor = jnp.minimum(1.0, 0.5 * lax.rsqrt(total / COUNT + 1e-30))
        factor_ref[...] = factor
        for one in loads:
            one.wait()

        @pl.loop(0, rows // tile)
        def _(t):
            at = pl.ds(pl.multiple_of(t * tile, tile), tile)
            out_ref[at] = updated(factor[:1, :1], held_g[at], held_m[at], held_v[at], held_w[at])

    return pl.pallas_call(
        kernel,
        in_specs=[pl.BlockSpec(memory_space=pltpu.SMEM), *(ANY,) * 4],
        out_specs=[pl.BlockSpec(memory_space=pltpu.VMEM)] * 2,
        out_shape=[jax.ShapeDtypeStruct((8, 128), F32), jax.ShapeDtypeStruct((rows, columns), BF16)],
        scratch_shapes=[
            pltpu.VMEM((rows, columns), BF16),
            pltpu.VMEM((rows, columns), F32),
            pltpu.VMEM((rows, columns), F32),
            pltpu.VMEM((rows, columns), BF16),
            pltpu.VMEM((8, 128), F32),
            pltpu.VMEM((DP - 1, 8, 128), F32),
            pltpu.SemaphoreType.DMA((4,)),
            pltpu.SemaphoreType.DMA((DP - 1,)),
            pltpu.SemaphoreType.DMA((DP - 1,)),
        ],
        compiler_params=pltpu.CompilerParams(vmem_limit_bytes=VMEM_LIMIT, collective_id=ident, has_side_effects=True),
        cost_estimate=cost(0.1, 10e6),
    )(squares.reshape(1), g, m, v, w)


def updated(factor, g, m, v, w):
    g = g.astype(F32) * factor
    m = 0.9 * m + 0.1 * g
    v = 0.95 * v + 0.05 * g * g
    w = w.astype(F32)
    return (w - 0.02 * (m * lax.rsqrt(v + 1e-8) + 0.1 * w)).astype(BF16)


def new_weight(layer, me, factor, g, m, v, w, full):
    rows, columns = g.shape
    steps = 4
    tile = rows // steps
    n_full = full is not None

    def kernel(me_ref, factor_ref, g_ref, m_ref, v_ref, w_ref, *rest):
        out_ref, full_ref = rest[n_full:]
        factor = factor_ref[:1, :1]

        @pl.loop(0, tile // 16)
        def _(t):
            at = pl.ds(pl.multiple_of(t * 16, 16), 16)
            out_ref[at] = full_ref[at] = updated(factor, g_ref[at], m_ref[at], v_ref[at], w_ref[at])

    mine = pl.BlockSpec((tile, columns), lambda i, _: (i, 0))
    state = pl.BlockSpec((None, tile, columns), lambda i, _: (layer, i, 0))
    own = pl.BlockSpec((None, tile, columns), lambda i, me_ref: (layer, me_ref[0] * steps + i, 0))
    return pl.pallas_call(
        kernel,
        grid_spec=pltpu.PrefetchScalarGridSpec(
            num_scalar_prefetch=1,
            grid=(steps,),
            in_specs=[whole((8, 128)), mine, state, state, own, *(ANY,) * n_full],
            out_specs=[mine, own],
        ),
        out_shape=[jax.ShapeDtypeStruct((rows, columns), BF16), jax.ShapeDtypeStruct(w.shape, BF16)],
        input_output_aliases={6: 1} if n_full else {},
        compiler_params=params(),
        cost_estimate=cost(0.1, 10e6),
    )(me.reshape(1), factor, g, m, v, w, *((full,) if n_full else ()))


def middle(ident, act_t, dg, du, w_gate, w_up, h, by_out, after):
    tile, half, rows_w, rest_columns = 512, 256, FF // DP, D // 4
    inner = D - rest_columns
    steps = T // tile
    n_after = len(after)

    def kernel(act_ref, by_ref, dg_ref, du_ref, wg_hbm, wu_hbm, h_ref, *rest):
        rest = rest[n_after:]
        out_ref, sum_ref, far_ref, near_ref, wg, wu, out, got, far, near, landed, load, send_sem, recv_sem, over_send, over_recv = rest
        i = pl.program_id(0)
        _, _, sib, opposite = peers()
        barrier = pltpu.get_barrier_semaphore()
        loads = [
            pltpu.make_async_copy(wg_hbm.at[1], wg, load.at[0]),
            pltpu.make_async_copy(wu_hbm.at[1], wu, load.at[1]),
        ]

        def beside(k):
            return remote(out.at[k], got.at[k], send_sem.at[k], recv_sem.at[k], sib)

        def over():
            return remote(far, landed, over_send.at[0], over_recv.at[0], opposite)

        @pl.when(i == 0)
        def _():
            for one in loads:
                one.start()
            for other in (sib, opposite):
                pl.semaphore_signal(barrier, inc=1, device_id={"dp": other}, device_id_type=MESH)

        @pl.when(i == 1)
        def _():
            pl.semaphore_wait(barrier, 2)
            beside(0).start()

        @pl.when(i == 2)
        def _():
            over().start()

        @pl.when(i == 3)
        def _():
            beside(1).start()

        @pl.when(i == DP)
        def _():
            for one in loads:
                one.wait()

        @pl.when(i < DP)
        def _():
            term = dot(act_ref[...], by_ref[...]).astype(BF16)

            @pl.when(i == 0)
            def _():
                out[0] = term

            @pl.when(i == 1)
            def _():
                beside(0).wait()
                there = (term.astype(F32) + got[0].astype(F32)).astype(BF16)
                far[...] = there[:, :inner]
                far_ref[...] = there[:, inner:]

            @pl.when(i == 2)
            def _():
                out[1] = term

            @pl.when(i == 3)
            def _():
                beside(1).wait()
                here = term.astype(F32) + got[1].astype(F32)
                near[...] = here[:, :inner]
                near_ref[...] = here[:, inner:]

        @pl.when(i >= DP)
        def _():
            for t in range(0, tile, half):
                rows = slice(t, t + half)
                by_a = dot_t(dg_ref[rows], wg[...]).astype(BF16) + dot_t(du_ref[rows], wu[...]).astype(BF16)
                c, wide = by_a.astype(F32), h_ref[rows].astype(F32)
                scale = root_mean_scale(wide)
                along = jnp.sum(c * wide, -1, keepdims=True)
                by = by_ref[pl.ds(pl.multiple_of((i - DP) * tile + t, half), half)]
                out_ref[rows] = by + (c * scale - wide * (scale * scale * scale * along * (1.0 / D))).astype(BF16)

        @pl.when(i == DP + steps - 1)
        def _():
            over().wait()
            sum_ref[...] = (near[...] + landed[...].astype(F32)).astype(BF16)

    def row(i):
        return jnp.maximum(i - DP, 0)

    def source(i):
        k = jnp.minimum(i, DP - 1)
        return block_of(lax.rem(k, CORES) * CORES + k // CORES)

    long = pl.BlockSpec((tile, FF), lambda i: (row(i), 0))
    short = pl.BlockSpec((tile, D), lambda i: (row(i), 0))
    most, few = (rows_w, inner), (rows_w, rest_columns)
    return pl.pallas_call(
        kernel,
        grid=(DP + steps,),
        in_specs=[pl.BlockSpec((rows_w, T), lambda i: (source(i), 0)), whole((T, D)), long, long, ANY, ANY, short, *(ANY,) * n_after],
        out_specs=[short, whole(most), whole(few), whole(few)],
        out_shape=[
            jax.ShapeDtypeStruct((T, D), BF16),
            jax.ShapeDtypeStruct(most, BF16),
            jax.ShapeDtypeStruct(few, BF16),
            jax.ShapeDtypeStruct(few, F32),
        ],
        scratch_shapes=[
            pltpu.VMEM((D, FF), BF16),
            pltpu.VMEM((D, FF), BF16),
            pltpu.VMEM((CORES, rows_w, D), BF16),
            pltpu.VMEM((CORES, rows_w, D), BF16),
            pltpu.VMEM(most, BF16),
            pltpu.VMEM(most, F32),
            pltpu.VMEM(most, BF16),
            *(pltpu.SemaphoreType.DMA((CORES,)),) * 3,
            *(pltpu.SemaphoreType.DMA((1,)),) * 2,
        ],
        compiler_params=remote_params(ident),
        cost_estimate=cost(3, 70e6),
    )(act_t, by_out, dg, du, w_gate, w_up, h, *after)


def solution(mesh):
    sibling = [(i, i ^ 1) for i in range(DP)]
    across = [(i, i ^ 2) for i in range(DP)]

    def step(x, dy, w_gate, w_up, w_down, m_gate, m_up, m_down, v_gate, v_up, v_down):
        x, dy = x[0], dy[0]
        me = lax.axis_index("dp")
        weights = (w_gate, w_up, w_down)

        def cross(far):
            return lax.ppermute(far, "dp", across)

        g1, u1, a1, h1, a2 = forward_first(x, *weights)
        units = {}
        sum_b, far, near, act2, dg2, du2 = hidden(0, 1, 8, 6, False, a2, dy, weights, None, ())
        units["b"] = near, cross(far)
        dh1, sum_d, far, near = middle(1, act2, dg2, du2, w_gate, w_up, h1, dy, (far,))
        units["d"] = near, cross(far)
        sum_e, far, near, act1 = hidden(2, 0, 6, 6, True, a1, dh1, weights, (g1, u1), ())
        units["e"] = near, cross(far)
        parts = ((0, 7 * D // 8), (7 * D // 8, D))
        *fars, near = down_grad(3, act1, dh1, parts, (far,))
        for k, (far, (start, stop)) in enumerate(zip(fars, parts, strict=True)):
            units[f"f{k}"] = near[:, start:stop], cross(far)

        nears = {name: near for name, (near, _) in units.items()}
        nears, inners, _ = lax.optimization_barrier((nears, {"b": sum_b, "d": sum_d, "e": sum_e}, fars))
        units = {name: (nears[name], landed) for name, (_, landed) in units.items()}
        grads, squared = {}, []
        for name, (near, landed) in units.items():
            grads[name] = (near + landed.astype(F32)).astype(BF16)
            squared.append(jnp.sum(grads[name].astype(F32) ** 2))
            if name in inners:
                squared.append(jnp.sum(inners[name].astype(F32) ** 2))
                grads[name] = jnp.concatenate([inners[name], grads[name]], -1)

        def of(which, layer):
            if which == 2:
                return grads["d"] if layer else jnp.concatenate([grads["f0"], grads["f1"]], 1)
            return grads["b" if layer else "e"][which]

        each = {(which, layer): of(which, layer) for which in range(3) for layer in range(2)}
        late = each.pop((2, 0))
        squares, each = lax.optimization_barrier((sum(squared), each))
        each[2, 0] = late

        ms, vs = (m_gate, m_up, m_down), (v_gate, v_up, v_down)
        full, sent = [None] * 3, []
        for (which, layer), g in sorted(each.items(), key=lambda one: one[0]):
            name = f"{which}{layer}"
            if not sent:
                factor, mine = clip_and_first(4, squares, g, ms[which], vs[which], weights[which])
            else:
                mine, full[which] = new_weight(layer, me, factor, g, ms[which], vs[which], weights[which], full[which])
            first = mine if which + layer == 0 else first
            over = lax.ppermute(mine, "dp", across)
            beside = lax.ppermute(mine, "dp", sibling)
            sent.append((which, layer, over, beside))
        factor, _ = lax.optimization_barrier((factor[0, 0], mine))
        new_m, new_v = [], []
        for which in range(3):
            g = jnp.stack([each[which, 0], each[which, 1]]).astype(F32) * factor
            new_m.append(0.9 * ms[which] + 0.1 * g)
            new_v.append(0.95 * vs[which] + 0.05 * g * g)
        for k, (which, layer, over, beside) in enumerate(sent):
            if 1 <= k <= 3:
                full, new_m[k - 1], new_v[k - 1] = lax.optimization_barrier((full, new_m[k - 1], new_v[k - 1]))

            def put(piece, who):
                full[which] = lax.dynamic_update_slice(full[which], piece[None], (layer, who * piece.shape[0], 0))

            if k == 0:
                put(first, me)
            put(beside, me ^ 1)
            over, full = lax.optimization_barrier((over, full))
            corner = lax.ppermute(over, "dp", sibling)
            put(over, me ^ 2)
            put(corner, me ^ 3)
        return (*full, *new_m, *new_v)

    batch, replicated, rows = P(("rep", "dp"), None, None), P(None, None, None), P(None, "dp", None)
    return jax.shard_map(
        step,
        mesh=mesh,
        in_specs=(batch, batch, *(replicated,) * 3, *(rows,) * 6),
        out_specs=(*(P("rep", None, None),) * 3, *(P("rep", "dp", None),) * 6),
        check_vma=False,
    )
```
